32 devices in a mesh: lon: 8 (over y, x, core), lev: 4 (over z).
Axes of the slice: x: 2, y: 2, z: 4, core: 2. Of those that a mesh axis runs over, the one named last changes fastest.
Arguments:
- field: float32 [72, 128, 128], P('lev', 'lon'), may hold values from -6 to 6
- ens: bfloat16 [80, 72, 128, 128], P(None, 'lev', 'lon'), may hold values from -2 to 2
- sdev: float32 [72, 128, 128], P('lev', 'lon'), may hold values from 0.5 to 2
- lon_taper: bfloat16 [17], replicated, may hold values from 0 to 0.079589844
- static_taper: bfloat16 [17], replicated, may hold values from 0 to 0.079589844
- loc_vert: bfloat16 [72, 72], P('lev'), may hold values from -0.75 to 0.75
- static_vert: bfloat16 [72, 72], P('lev'), may hold values from -0.75 to 0.75
- obs_block: int32 [8192], P('lon'), may hold values from -1 to 127, as said below
- obs_value: float32 [8192], P('lon'), may hold values from -6 to 6
- obs_rinv: float32 [8192], P('lon'), may hold values from 0.25 to 4
- obs_horiz: float32 [8192, 128], P('lon'), may hold values from -0.5 to 0.5
- obs_vert: float32 [8192, 72], P('lon', 'lev'), may hold values from -0.75 to 0.75
Outputs:
- increment: float32 [72, 128, 128], P('lev', 'lon')
- adjoint_field: float32 [72, 128, 128], P('lev', 'lon')
- obs_cost: float32 [], replicated
The draws below stay inside these ranges and needn't reach their ends.
Inputs may be any that keep to these rules, and one draw needn't show every extreme that they name: `obs_block`: each longitude sector's 1024 slots name only blocks within that sector's longitudes; live slots come first, in non-falling block order; at least half of a sector's slots are live, and some sector has all its slots live.
All inputs are finite; a program needn't handle non-finite values.
Results may differ from the reference program's by a relative error of at most 0.0041.
Values may be sent and summed in bfloat16 or wider, within the bound.
No kernel may reach another device: no remote copies, remote signals or barrier semaphores. Data moves between devices by JAX's collectives and lax.ppermute only.
A program may use at most 128 MiB of HBM per device.

```python
import math
import jax
import jax.numpy as jnp
from jax import lax

ENS = 80
LEV = 72
LAT = 128
LON_DEV = 16
OBS_DEV = 1024
HALO = 8
NLON = 128
NOBS = 8192


def draw_obs_block(key, part):
    groups = NOBS // OBS_DEV
    per_group = LON_DEV // 8 * (LAT // 16)
    key_ids = jax.random.fold_in(key, 11)
    key_live = jax.random.fold_in(key, 23)
    local = jnp.sort(jax.random.randint(key_ids, (groups, OBS_DEV), 0, per_group), axis=1)
    counts = jax.random.randint(key_live, (groups, 1), OBS_DEV // 2, OBS_DEV + 1)
    counts = counts.at[0, 0].set(OBS_DEV)
    slots = jnp.arange(OBS_DEV)[None, :]
    base = jnp.arange(groups)[:, None] * per_group
    ids = jnp.where(slots < counts, local + base, -1)
    return ids.reshape(-1).astype(jnp.int32)


def steps_of(stream_key, dims, shards, least, high):
    level, own = 1.0, jax.random.fold_in(stream_key, 6)
    for position, blocks in shards:
        steps = jnp.exp(jax.random.uniform(jax.random.fold_in(own, position), (blocks,), jnp.float32, least / len(shards), high / len(shards)))
        level = level * jnp.repeat(steps, dims[position] // blocks).reshape([-1 if axis == position else 1 for axis in range(len(dims))])
    return level


def noise(rng, dims, spread, most, cuts=(), dtype=jnp.bfloat16):
    entries = spread * jax.random.normal(rng, dims, jnp.float32)
    if cuts:
        entries = entries * steps_of(rng, dims, cuts, -0.22, 0.18)
    return jnp.clip(entries, -most, most).astype(dtype)


def setup_inputs(seed: int = 0) -> dict:
    key_list = jax.random.split(jax.random.key(seed), 13)
    field = noise(key_list[0], (LEV, NLON, LAT), 1.0, 6.0, ((0, 4), (1, 8)), jnp.float32)
    ens = noise(key_list[1], (ENS, LEV, NLON, LAT), 0.3, 2.0, ((1, 4), (2, 8)))
    sdev = jnp.clip(jnp.exp(math.log(2.0) - 1.3862944 * jax.random.uniform(key_list[2], (LEV, NLON, LAT), jnp.float32) ** steps_of(key_list[2], (LEV, NLON, LAT), ((0, 4), (1, 8)), -0.2, 0.2)), 0.5, 2.0)
    lon_taper = jnp.clip(jax.random.uniform(key_list[3], (2 * HALO + 1,), jnp.float32, 0.0, 0.079589844), 0.0, 0.079589844).astype(jnp.bfloat16)
    static_taper = jnp.clip(jax.random.uniform(key_list[4], (2 * HALO + 1,), jnp.float32, 0.0, 0.079589844), 0.0, 0.079589844).astype(jnp.bfloat16)
    loc_vert = noise(key_list[5], (LEV, LEV), LEV ** -0.5, 0.75, ((0, 4),))
    static_vert = noise(key_list[6], (LEV, LEV), LEV ** -0.5, 0.75, ((0, 4),))
    obs_block = draw_obs_block(jax.random.fold_in(key_list[12], 71), 0)
    obs_value = noise(key_list[8], (NOBS,), 1.0, 6.0, ((0, 8),), jnp.float32)
    obs_rinv = jnp.clip(jnp.exp(math.log(4.0) - 2.7725887 * jax.random.uniform(key_list[9], (NOBS,), jnp.float32) ** steps_of(key_list[9], (NOBS,), ((0, 8),), -0.2, 0.2)), 0.25, 4.0)
    obs_horiz = noise(key_list[10], (NOBS, 128), 128 ** -0.5, 0.5, ((0, 8),), jnp.float32)
    obs_vert = noise(key_list[11], (NOBS, LEV), LEV ** -0.5, 0.75, ((0, 8), (1, 4)), jnp.float32)
    return dict(field=field, ens=ens, sdev=sdev, lon_taper=lon_taper, static_taper=static_taper, loc_vert=loc_vert, static_vert=static_vert, obs_block=obs_block, obs_value=obs_value, obs_rinv=obs_rinv, obs_horiz=obs_horiz, obs_vert=obs_vert)


ens_weight = 0.8
static_weight = 0.5


def localize(zfield, taper, vmatrix):
    width = taper.shape[0]
    half = width // 2
    total = jnp.zeros(zfield.shape, jnp.float32)
    for offset in range(width):
        total = total + taper[offset].astype(jnp.float32) * jnp.roll(zfield, half - offset, axis=1).astype(jnp.float32)
    smooth = total.astype(jnp.bfloat16)
    levels = smooth.shape[0]
    flat = smooth.reshape(levels, -1)
    return jnp.dot(vmatrix, flat, preferred_element_type=jnp.float32).reshape(zfield.shape)


def reference(field, ens, sdev, lon_taper, static_taper, loc_vert, static_vert, obs_block, obs_value, obs_rinv, obs_horiz, obs_vert):
    def member(total, pert):
        zpert = (pert.astype(jnp.float32) * field).astype(jnp.bfloat16)
        return total + pert.astype(jnp.float32) * localize(zpert, lon_taper, loc_vert), None

    ens_sum, _ = lax.scan(member, jnp.zeros(field.shape, jnp.float32), ens)
    spart = (sdev * field).astype(jnp.bfloat16)
    static_sum = localize(spart, static_taper, static_vert)
    increment = ens_weight * ens_sum + static_weight * sdev * static_sum
    nblk = (NLON // 8) * (LAT // 16)
    blocks = increment.reshape(LEV, NLON // 8, 8, LAT // 16, 16).transpose(0, 1, 3, 2, 4).reshape(LEV, nblk, 128)
    groups = NOBS // OBS_DEV
    ids = obs_block.reshape(groups, OBS_DEV)
    values = obs_value.reshape(groups, OBS_DEV)
    rinv = obs_rinv.reshape(groups, OBS_DEV)
    horiz = obs_horiz.reshape(groups, OBS_DEV, 128)
    vert = obs_vert.reshape(groups, OBS_DEV, LEV)

    def observe(carry, items):
        block_ids, value, weight, hpart, vpart = items
        live = block_ids >= 0
        safe = jnp.where(live, block_ids, 0).astype(jnp.int32)
        picked = jnp.take(blocks, safe, axis=1)
        hz = jnp.einsum('ljc,jc->lj', picked, hpart, precision=lax.Precision.HIGHEST)
        hx = jnp.einsum('jl,lj->j', vpart, hz, precision=lax.Precision.HIGHEST)
        miss = hx - value
        dep = jnp.where(live, weight * miss, 0.0)
        cost = 0.5 * jnp.sum(dep * miss)
        terms = (dep[:, None, None] * vpart[:, :, None]) * hpart[:, None, :]
        adj = jax.ops.segment_sum(terms, safe, num_segments=nblk)
        return (carry[0] + adj, carry[1] + cost), None

    init = (jnp.zeros((nblk, LEV, 128), jnp.float32), jnp.zeros((), jnp.float32))
    (adj_blocks, obs_cost), _ = lax.scan(observe, init, (ids, values, rinv, horiz, vert))
    adjoint_field = adj_blocks.transpose(1, 0, 2).reshape(LEV, NLON // 8, LAT // 16, 8, 16).transpose(0, 1, 3, 2, 4).reshape(LEV, NLON, LAT)
    return increment, adjoint_field, obs_cost
```

```python
import functools

import jax
import jax.numpy as jnp
from jax import lax
from jax.experimental import pallas as pl
from jax.experimental.pallas import tpu as pltpu
from jax.sharding import PartitionSpec as P


ens_weight = 0.8
static_weight = 0.5
block_lon = 8
block_lat = 16
f32 = jnp.float32
bf16 = jnp.bfloat16


def shift_by(axis, amount):
    count = lax.axis_size(axis)
    return [(i, (i + amount) % count) for i in range(count)]


def vmem():
    return pl.BlockSpec(memory_space=pltpu.VMEM)


def anywhere():
    return pl.BlockSpec(memory_space=pl.ANY)


def params(count=0):
    return pltpu.CompilerParams(vmem_limit_bytes=(24 if count <= 2 else 58) * 2**20)


def smem():
    return pl.BlockSpec(memory_space=pltpu.SMEM)


def cost(flops, nbytes):
    return pl.CostEstimate(flops=int(flops), bytes_accessed=int(nbytes), transcendentals=0)


def lane_groups(shape, width):
    return lax.broadcasted_iota(jnp.int32, shape, len(shape) - 1) // width


def regroup(sources, quarter, parts, width):
    group = lane_groups(sources[0].shape, width)
    out = None
    for p, source in enumerate(sources):
        turn = lax.rem(p - quarter + parts, parts) * width
        moved = pltpu.roll(source, turn, source.ndim - 1)
        out = moved if out is None else jnp.where(group == p, moved, out)
    return out


def pack_kernel(parts, halves, me_ref, ens_ref, after, *outs):
    levels, columns, lanes = ens_ref.shape[1:]
    width = lanes // parts
    rows = columns // halves
    me = me_ref[0]
    sources = [ens_ref[p].astype(f32).reshape(levels * columns, lanes) for p in range(parts)]
    for s, out in enumerate(outs):
        packed = regroup(sources, lax.rem(me + s, parts), parts, width)
        packed = packed.reshape(levels, halves, rows, lanes)
        for h in range(halves):
            out[0, h] = packed[:, h].reshape(levels * rows, lanes).astype(bf16)


def pack(me, ens, start, count, parts, halves, after):
    _, levels, columns, lanes = ens.shape
    rows = levels * columns // halves
    shape = jax.ShapeDtypeStruct((count, halves, rows, lanes), bf16)
    return pl.pallas_call(
        functools.partial(pack_kernel, parts, halves),
        grid=(count,),
        in_specs=[
            smem(),
            pl.BlockSpec((parts, levels, columns, lanes), lambda i: (start + i, 0, 0, 0)),
            anywhere(),
        ],
        out_specs=[pl.BlockSpec((1, halves, rows, lanes), lambda i: (i, 0, 0, 0))] * parts,
        out_shape=[shape] * parts,
        cost_estimate=cost(count * 4e6, count * parts * halves * rows * lanes * 4),
        compiler_params=params(8),
        name="pack",
    )(me, ens, after)


def ceil_to(x, unit):
    return -(-x // unit) * unit


def message_rows(levels, half_rows, slots, lanes):
    vert = 2 * half_rows
    loc = vert + ceil_to(levels * slots // lanes, 16)
    stat = loc + ceil_to(levels, 16)
    return 0, half_rows, vert, loc, stat, stat + ceil_to(levels, 16)


def pack_small_kernel(
    parts, halves, first, me_ref, field_ref, sdev_ref, vert_ref, loc_ref, stat_ref, after, *outs
):
    levels, columns, lanes = field_ref.shape
    width = lanes // parts
    rows = columns // halves
    slots = vert_ref.shape[0]
    me = me_ref[0]
    sources = []
    for h in range(halves):
        for ref in (field_ref, sdev_ref):
            sources.append(ref[:, h * rows : (h + 1) * rows, :].reshape(levels * rows, lanes))
    flat = vert_ref[...].T
    flat = jnp.concatenate(
        [flat[:, t : t + lanes] for t in range(0, slots, lanes)], axis=0
    ).astype(bf16)
    for s, out in enumerate(outs):
        high, low = split(regroup(sources, lax.rem(me + s, parts), parts, width))
        out[first[0] : first[1], :] = high
        out[first[1] : first[2], :] = low
        out[first[2] : first[2] + flat.shape[0], :] = flat
        for begin, ref in ((first[3], loc_ref), (first[4], stat_ref)):
            out[begin : begin + ceil_to(levels, 16), :] = jnp.zeros(
                (ceil_to(levels, 16), lanes), bf16
            )
            out[begin : begin + levels, : ref.shape[1]] = ref[...]


def pack_small(me, field, sdev, vert, loc, stat, parts, halves, after):
    levels, columns, lanes = field.shape
    first = message_rows(levels, levels * columns // halves, vert.shape[0], lanes)
    return pl.pallas_call(
        functools.partial(pack_small_kernel, parts, halves, first),
        in_specs=[smem()] + [vmem()] * 5 + [anywhere()],
        out_specs=[vmem()] * parts,
        out_shape=[jax.ShapeDtypeStruct((first[-1], lanes), bf16)] * parts,
        compiler_params=params(),
        name="pack_small",
    )(me, field, sdev, vert, loc, stat, after)


def spread_kernel(parts, halves, levels, first, after, *refs):
    messages, (wide_field, wide_sdev, left_end, right_end, vert, loc, stat) = (
        refs[:parts],
        refs[parts:],
    )
    rows = wide_field.shape[1] // parts
    lanes = messages[0].shape[1]
    width = lanes // parts
    group = lane_groups((rows, lanes), width)
    ends = (left_end, right_end)
    for s, message in enumerate(messages):
        x = message[:rows, :].astype(f32) + message[rows : 2 * rows, :].astype(f32)
        for h in range(halves):
            wide = []
            for t in range(2):
                one = jnp.where(group == 2 * h + t, x, 0.0)
                both = one
                for k in range(1, parts):
                    both = both + pltpu.roll(one, k * width, 1)
                wide.append(both)
            wide_field[h, s * rows : (s + 1) * rows, :] = wide[0]
            wide_sdev[h, s * rows : (s + 1) * rows, :] = wide[1]
            ends[h][0, s * rows : (s + 1) * rows, :] = (wide[0] * wide[1]).astype(bf16)
        here = slice(s * levels, (s + 1) * levels)
        count = vert.shape[1] // lanes
        x = message[first[2] : first[2] + count * levels, :].astype(f32)
        for t in range(count):
            vert[here, t * lanes : (t + 1) * lanes] = x[t * levels : (t + 1) * levels]
    for begin, out in ((first[3], loc), (first[4], stat)):
        out[...] = jnp.concatenate(
            [m[begin : begin + ceil_to(levels, 16), :].astype(f32)[:levels] for m in messages],
            axis=0,
        ).astype(bf16)


def spread(messages, levels, rows, slots, parts, halves, after):
    lanes = messages[0].shape[1]
    first = message_rows(levels, rows, slots, lanes)
    wide = jax.ShapeDtypeStruct((halves, parts * rows, lanes), f32)
    end = jax.ShapeDtypeStruct((1, parts * rows, lanes), bf16)
    matrix = jax.ShapeDtypeStruct((parts * levels, lanes), bf16)
    vert = jax.ShapeDtypeStruct((parts * levels, slots), f32)
    return pl.pallas_call(
        functools.partial(spread_kernel, parts, halves, levels, first),
        in_specs=[anywhere()] + [vmem()] * parts,
        out_specs=[vmem()] * 7,
        out_shape=[wide, wide, end, end, vert, matrix, matrix],
        compiler_params=params(),
        name="spread",
    )(after, *messages)


def product_kernel(parts, field_ref, after, *refs):
    xs, ends = refs[:parts], refs[parts:]
    count, _, rows, _ = xs[0].shape
    for s, x in enumerate(xs):
        here = slice(s * rows, (s + 1) * rows)
        for h, end in enumerate(ends):
            scale = field_ref[h, here, :]
            for k in range(count):
                end[k, here, :] = (x[k, h].astype(f32) * scale).astype(bf16)


def product(wide_field, xs, after):
    parts = len(xs)
    count, halves, rows, lanes = xs[0].shape
    step = 2 if count % 2 == 0 else 1
    end = jax.ShapeDtypeStruct((count, parts * rows, lanes), bf16)
    return pl.pallas_call(
        functools.partial(product_kernel, parts),
        grid=(count // step,),
        in_specs=[pl.BlockSpec(wide_field.shape, lambda i: (0, 0, 0)), anywhere()]
        + [pl.BlockSpec((step, halves, rows, lanes), lambda i: (i, 0, 0, 0))] * parts,
        out_specs=[pl.BlockSpec((step, parts * rows, lanes), lambda i: (i, 0, 0))] * halves,
        out_shape=[end] * halves,
        cost_estimate=cost(count * 1e6, count * halves * parts * rows * lanes * 4),
        compiler_params=params(count),
        name="product",
    )(wide_field, after, *xs)


def filter_kernel(pair, has_total, matrix_ref, left, first, last, right, *refs):
    refs = list(refs)
    stack = refs.pop()
    total_out = refs.pop()
    total_in = refs.pop() if has_total else None
    xs = refs
    rows, lanes = first.shape[1:]

    @pl.when(pl.program_id(0) == 0)
    def _():
        if has_total:
            total_out[...] = total_in[...]
        else:
            total_out[...] = jnp.zeros_like(total_out)

    for n, ref in enumerate((left, first, last, right)):
        for k in range(pair):
            stack[n * rows : (n + 1) * rows, k * lanes : (k + 1) * lanes] = ref[k]
    for h in range(total_out.shape[0]):
        y = jnp.dot(
            matrix_ref[...], stack[h * rows : (h + 3) * rows, :], preferred_element_type=f32
        )
        piece = rows // len(xs)
        for s, x in enumerate(xs):
            here = slice(s * piece, (s + 1) * piece)
            add = total_out[h, here, :]
            for k in range(pair):
                add = add + x[k, h].astype(f32) * y[here, k * lanes : (k + 1) * lanes]
            total_out[h, here, :] = add


def filtered(matrix, left, first, last, right, xs, total):
    count, rows, lanes = first.shape
    pair = 2 if count % 2 == 0 else 1
    halves = 2
    piece = rows // len(xs)
    edge = pl.BlockSpec((pair, rows, lanes), lambda i: (i, 0, 0))
    whole = pl.BlockSpec((halves, rows, lanes), lambda i: (0, 0, 0))
    return pl.pallas_call(
        functools.partial(filter_kernel, pair, total is not None),
        grid=(count // pair,),
        in_specs=[pl.BlockSpec(matrix.shape, lambda i: (0, 0))]
        + [edge] * 4
        + [pl.BlockSpec((pair, halves, piece, lanes), lambda i: (i, 0, 0, 0))] * len(xs)
        + ([whole] if total is not None else []),
        out_specs=whole,
        out_shape=jax.ShapeDtypeStruct((halves, rows, lanes), f32),
        scratch_shapes=[pltpu.VMEM((4 * rows, pair * lanes), bf16)],
        cost_estimate=cost(
            2 * halves * matrix.shape[0] * matrix.shape[1] * lanes * count,
            count * rows * lanes * 12,
        ),
        compiler_params=params(count),
        name="filtered",
    )(matrix, left, first, last, right, *xs, *([total] if total is not None else []))


def fold_kernel(parts, block_rows, total_ref, static_ref, blocks_ref, mixed):
    halves, rows, lanes = total_ref.shape
    width = lanes // parts
    levels = rows // block_lon
    for h in range(halves):
        x = ens_weight * total_ref[h] + (static_weight / parts) * static_ref[h]
        folded = x
        for k in range(1, parts):
            folded = folded + pltpu.roll(x, k * width, 1)
        mixed[h * rows : (h + 1) * rows, :] = folded
    group = lane_groups((levels, lanes), block_lat)
    for h in range(halves):
        strips = [mixed[pl.ds(h * rows + i, levels, stride=block_lon), :] for i in range(block_lon)]
        for b in range(block_rows):
            out = None
            for i, strip in enumerate(strips):
                moved = pltpu.roll(strip, ((i - b) * block_lat) % lanes, 1)
                out = moved if out is None else jnp.where(group == i, moved, out)
            blocks_ref[b, h * levels : (h + 1) * levels, :] = out


def fold(total, static, parts):
    halves, rows, lanes = total.shape
    levels = rows // block_lon
    block_rows = lanes // parts // block_lat
    return pl.pallas_call(
        functools.partial(fold_kernel, parts, block_rows),
        in_specs=[vmem()] * 2,
        out_specs=vmem(),
        out_shape=jax.ShapeDtypeStruct((block_rows, halves * levels, lanes), f32),
        scratch_shapes=[pltpu.VMEM((halves * rows, lanes), f32)],
        cost_estimate=cost(2e6, 2e6),
        compiler_params=params(),
        name="fold",
    )(total, static)


def split(x):
    high = x.astype(bf16)
    return high, (x - high.astype(f32)).astype(bf16)


def horiz_kernel(horiz_ref, high, low, high_t, low_t):
    hi, lo = split(horiz_ref[...])
    high[...] = hi
    low[...] = lo
    flipped_hi, flipped_lo = split(horiz_ref[...].T)
    high_t[...] = flipped_hi
    low_t[...] = flipped_lo


def horiz_parts(horiz):
    slots, cells = horiz.shape
    return pl.pallas_call(
        horiz_kernel,
        in_specs=[vmem()],
        out_specs=[vmem()] * 4,
        out_shape=[jax.ShapeDtypeStruct((slots, cells), bf16)] * 2
        + [jax.ShapeDtypeStruct((cells, slots), bf16)] * 2,
        cost_estimate=cost(1e6, 2e6),
        compiler_params=params(),
        name="horiz_parts",
    )(horiz)


def product3(a, high, low):
    a_high, a_low = split(a)
    dot = functools.partial(jnp.dot, preferred_element_type=f32)
    return dot(a_high, high) + (dot(a_low, high) + dot(a_high, low))


def observe_kernel(
    parts, halves, lat_blocks, me_ref, blocks_ref, vert_ref, high, low, high_t, low_t,
    ids_ref, value_ref, rinv_ref, *outs
):
    block_rows, stacked, cells = blocks_ref.shape
    levels = stacked // halves
    piece = levels // parts
    base = me_ref[0] * block_rows
    ids = ids_ref[...]
    vert = vert_ref[...]
    picks = [
        [ids == h * lat_blocks + base + b for b in range(block_rows)] for h in range(halves)
    ]
    mine = None
    hx = jnp.zeros(ids.shape, f32)
    for b in range(block_rows):
        projected = product3(blocks_ref[b], high_t[...], low_t[...])
        for h in range(halves):
            one = jnp.sum(projected[h * levels : (h + 1) * levels] * vert, axis=0, keepdims=True)
            hx = jnp.where(picks[h][b], one, hx)
            mine = picks[h][b] if mine is None else mine | picks[h][b]
    miss = hx - value_ref[...]
    dep = jnp.where(mine, rinv_ref[...] * miss, 0.0)
    total = 0.5 * jnp.sum(dep * miss, axis=1, keepdims=True)
    tile = (8, cells)
    spot = lax.broadcasted_iota(jnp.int32, tile, 0) * cells
    spot = spot + lax.broadcasted_iota(jnp.int32, tile, 1)
    share = jnp.where(spot == me_ref[1], jnp.broadcast_to(total, tile), 0.0)
    for ref in outs:
        ref[ref.shape[0] - 8 :, :] = share
    for b in range(block_rows):
        weights = jnp.concatenate(
            [vert * jnp.where(picks[h][b], dep, 0.0) for h in range(halves)], axis=0
        )
        adjoint = product3(weights, high[...], low[...])
        for h in range(halves):
            block = h * block_rows + b
            for s, ref in enumerate(outs):
                first = h * levels + s * piece
                count = piece * halves * block_rows
                where = pl.ds(block, piece, stride=halves * block_rows)
                ref[where, :] = blocks_ref[b, first : first + piece, :]
                where = pl.ds(count + block, piece, stride=halves * block_rows)
                ref[where, :] = adjoint[first : first + piece]


def observe(me, blocks, vert, horiz, ids, value, rinv, parts, halves, lat_blocks):
    block_rows, stacked, cells = blocks.shape
    back = jax.ShapeDtypeStruct((2 * block_rows * stacked // parts + 8, cells), f32)
    return pl.pallas_call(
        functools.partial(observe_kernel, parts, halves, lat_blocks),
        in_specs=[smem()] + [vmem()] * 9,
        out_specs=[vmem()] * parts,
        out_shape=[back] * parts,
        cost_estimate=cost(1e9, 4e6),
        compiler_params=params(),
        name="observe",
    )(me, blocks, vert, *horiz, ids, value, rinv)


def unpack(index, backs, levels, columns, lanes):
    parts = len(backs)
    halves = columns // block_lon
    block_rows = lanes // parts // block_lat
    used = 2 * levels * halves * block_rows
    twice = jnp.concatenate([x[None, :used] for x in backs + backs], axis=0)
    ordered = lax.dynamic_slice_in_dim(twice, (parts - index) % parts, parts, axis=0)
    ordered = ordered.reshape(parts, 2, levels, halves, block_rows, block_lon, block_lat)
    both = ordered.transpose(1, 2, 3, 5, 0, 4, 6).reshape(2, levels, columns, lanes)
    return both[0], both[1]


def exchange(blocks, axis, sign):
    return [blocks[0]] + [
        lax.ppermute(blocks[s], axis, shift_by(axis, sign * s)) for s in range(1, len(blocks))
    ]


def bands_kernel(rows, span, lon_ref, static_ref, *outs):
    for taper_ref, out in zip((lon_ref, static_ref), outs):
        column = lax.broadcasted_iota(jnp.int32, out.shape, 1)
        offset = column // span * rows + column % rows
        offset = offset - lax.broadcasted_iota(jnp.int32, out.shape, 0)
        band = jnp.zeros(out.shape, f32)
        for d in range(2 * rows + 1):
            band = jnp.where(offset == d, taper_ref[d], band)
        out[...] = band


def bands(lon_taper, static_taper, rows, span):
    shape = jax.ShapeDtypeStruct((rows, 3 * span), f32)
    return pl.pallas_call(
        functools.partial(bands_kernel, rows, span),
        in_specs=[smem()] * 2,
        out_specs=[vmem()] * 2,
        out_shape=[shape] * 2,
        compiler_params=params(),
        name="bands",
    )(lon_taper.astype(f32), static_taper.astype(f32))


def operator(vert_rows, band, me, parts, levels, rows):
    total = parts * levels
    span = total * rows
    column = jnp.arange(3 * span)
    source = column % span // rows
    owner = (me - source // levels) % parts
    pick = (jnp.arange(vert_rows.shape[1])[:, None] == (owner * levels + source % levels)[None, :])
    wide = jnp.dot(vert_rows, pick.astype(bf16), preferred_element_type=f32).astype(bf16)
    grow = (jnp.arange(span)[:, None] // rows == jnp.arange(total)[None, :]).astype(bf16)
    tall = jnp.dot(grow, wide, preferred_element_type=f32)
    return (tall.reshape(total, rows, 3 * span) * band[None]).astype(bf16).reshape(span, 3 * span)


def sent(packed):
    return exchange(packed, "lev", 1)


def chunk_sizes(groups):
    sizes = [2, 4, 4, 4, 4, 2]
    if sum(sizes) == groups:
        return sizes
    return [groups - groups // 2, groups // 2] if groups > 1 else [groups]


def body(
    field,
    ens,
    sdev,
    lon_taper,
    static_taper,
    loc_vert,
    static_vert,
    obs_block,
    obs_value,
    obs_rinv,
    obs_horiz,
    obs_vert,
):
    members, levels, columns, lanes = ens.shape
    parts = lax.axis_size("lev")
    rows = lon_taper.shape[0] // 2
    halves = columns // rows
    lat_blocks = lanes // block_lat
    slots = obs_block.shape[0]
    index = lax.axis_index("lev")
    me = jnp.stack([index, lax.axis_index("lon") * parts + index]).astype(jnp.int32)

    sizes = chunk_sizes(members // parts)
    starts = [sum(sizes[:n]) for n in range(len(sizes))]
    first_pack = pack(me, ens, starts[0], sizes[0], parts, halves, me)
    messages = pack_small(
        me, field, sdev, obs_vert, loc_vert, static_vert, parts, halves, first_pack[0]
    )
    half_rows = levels * rows
    received = [sent(first_pack)]
    after = messages[0]
    messages = exchange(messages, "lev", 1)
    for n in range(1, len(sizes)):
        packed = pack(me, ens, starts[n], sizes[n], parts, halves, after)
        after = packed[0]
        received.append(sent(packed))

    wide_field, wide_sdev, static_first, static_last, vert_all, loc_all, stat_all = spread(
        messages, levels, half_rows, slots, parts, halves, after
    )
    lon_band, static_band = bands(lon_taper, static_taper, rows, parts * half_rows)
    loc_matrix = operator(loc_all, lon_band, index, parts, levels, rows)
    stat_matrix = operator(stat_all, static_band, index, parts, levels, rows)
    horiz = horiz_parts(obs_horiz)

    def halo(first, last):
        left = lax.ppermute(last, "lon", shift_by("lon", 1))
        right = lax.ppermute(first, "lon", shift_by("lon", -1))
        return left, right

    left, right = halo(static_first, static_last)
    static = filtered(stat_matrix, left, static_first, static_last, right, [wide_sdev[None]], None)
    total = None
    ready = None
    after = static_first
    for xs in received:
        first, last = product(wide_field, xs, after)
        if ready is not None:
            total = filtered(loc_matrix, *ready, total)
            after = total
        else:
            after = static
        left, right = halo(first, last)
        ready = left, first, last, right, xs
    total = filtered(loc_matrix, *ready, total)

    blocks = fold(total, static, parts)

    nblk = columns // block_lon * lat_blocks
    ids = jnp.where(obs_block >= 0, obs_block - lax.axis_index("lon") * nblk, -1)
    backs = observe(
        me, blocks, vert_all, horiz, ids[None], obs_value[None], obs_rinv[None],
        parts, halves, lat_blocks,
    )
    backs = exchange(backs, "lev", -1)
    shares = sum(x[-8:] for x in backs)
    reach = 1
    while reach < lax.axis_size("lon"):
        pairs = [(i, i ^ reach) for i in range(lax.axis_size("lon"))]
        shares = shares + lax.ppermute(shares, "lon", pairs)
        reach *= 2
    obs_cost = jnp.sum(shares)

    increment, adjoint_field = unpack(index, backs, levels, columns, lanes)
    return (increment, adjoint_field, obs_cost)


def solution(mesh):
    return jax.shard_map(
        body,
        mesh=mesh,
        in_specs=(
            P("lev", "lon", None),
            P(None, "lev", "lon", None),
            P("lev", "lon", None),
            P(),
            P(),
            P("lev", None),
            P("lev", None),
            P("lon"),
            P("lon"),
            P("lon"),
            P("lon", None),
            P("lon", "lev"),
        ),
        out_specs=(P("lev", "lon", None), P("lev", "lon", None), P()),
        check_vma=False,
    )
```

```python
import functools

import jax
import jax.numpy as jnp
from jax import lax
from jax.experimental import pallas as pl
from jax.experimental.pallas import tpu as pltpu
from jax.sharding import PartitionSpec as P


ens_weight = 0.8
static_weight = 0.5
block_lon = 8
block_lat = 16
LIMIT = 44
plan = (2, 4, 4, 4, 2, 2, 2)
f32 = jnp.float32
bf16 = jnp.bfloat16


def my_partner(place):
    return lax.axis_index("lev") ^ place


def shift_by(axis, amount):
    count = lax.axis_size(axis)
    return [(i, (i + amount) % count) for i in range(count)]


def vmem():
    return pl.BlockSpec(memory_space=pltpu.VMEM)


def anywhere():
    return pl.BlockSpec(memory_space=pl.ANY)


def params(count=0):
    return pltpu.CompilerParams(vmem_limit_bytes=(58 if count > 20 else LIMIT) * 2**20)


def smem():
    return pl.BlockSpec(memory_space=pltpu.SMEM)


def cost(flops, nbytes):
    return pl.CostEstimate(flops=int(flops), bytes_accessed=int(nbytes), transcendentals=0)


def lane_groups(shape, width):
    return lax.broadcasted_iota(jnp.int32, shape, len(shape) - 1) // width


def regroup(sources, quarter, parts, width):
    group = lane_groups(sources[0].shape, width)
    out = None
    for p, source in enumerate(sources):
        turn = lax.rem(p - quarter + parts, parts) * width
        moved = pltpu.roll(source, turn, source.ndim - 1)
        out = moved if out is None else jnp.where(group == p, moved, out)
    return out


def pack_kernel(parts, halves, ens_ref, after, *outs):
    levels, columns, lanes = ens_ref.shape[1:]
    width = lanes // parts
    rows = columns // halves
    sources = [ens_ref[p].astype(f32).reshape(levels * columns, lanes) for p in range(parts)]
    for s, out in enumerate(outs):
        packed = regroup(sources, my_partner(s), parts, width)
        packed = packed.reshape(levels, halves, rows, lanes)
        for h in range(halves):
            out[0, h] = packed[:, h].reshape(levels * rows, lanes).astype(bf16)


def pack(ens, start, count, parts, halves, after):
    _, levels, columns, lanes = ens.shape
    rows = levels * columns // halves
    shape = jax.ShapeDtypeStruct((count, halves, rows, lanes), bf16)
    return pl.pallas_call(
        functools.partial(pack_kernel, parts, halves),
        grid=(count,),
        in_specs=[
            pl.BlockSpec((parts, levels, columns, lanes), lambda i: (start + i, 0, 0, 0)),
            anywhere(),
        ],
        out_specs=[pl.BlockSpec((1, halves, rows, lanes), lambda i: (i, 0, 0, 0))] * parts,
        out_shape=[shape] * parts,
        cost_estimate=cost(count * 4e6, count * parts * halves * rows * lanes * 4),
        compiler_params=params(99),
        name="pack",
    )(ens, after)


def ceil_to(x, unit):
    return -(-x // unit) * unit


def message_rows(levels, half_rows, slots, lanes):
    loc = 2 * half_rows
    stat = loc + ceil_to(levels, 16)
    return 0, half_rows, loc, stat, stat + ceil_to(levels, 16), levels * slots // lanes


def pack_small_kernel(
    parts, halves, first, field_ref, sdev_ref, vert_ref, loc_ref, stat_ref, after, *outs
):
    *outs, flat_ref = outs
    levels, columns, lanes = field_ref.shape
    width = lanes // parts
    rows = columns // halves
    slots = vert_ref.shape[0]
    sources = []
    for h in range(halves):
        for ref in (field_ref, sdev_ref):
            sources.append(ref[:, h * rows : (h + 1) * rows, :].reshape(levels * rows, lanes))
    flat = vert_ref[...].T
    flat_ref[...] = jnp.concatenate(
        [flat[:, t : t + lanes] for t in range(0, slots, lanes)], axis=0
    ).astype(bf16)
    for s, out in enumerate(outs):
        high, low = split(regroup(sources, my_partner(s), parts, width))
        out[first[0] : first[1], :] = high
        out[first[1] : first[2], :] = low
        for begin, ref in ((first[2], loc_ref), (first[3], stat_ref)):
            out[begin : begin + ceil_to(levels, 16), :] = jnp.zeros(
                (ceil_to(levels, 16), lanes), bf16
            )
            out[begin : begin + levels, : ref.shape[1]] = ref[...]


def pack_small(field, sdev, vert, loc, stat, parts, halves, after):
    levels, columns, lanes = field.shape
    first = message_rows(levels, levels * columns // halves, vert.shape[0], lanes)
    return pl.pallas_call(
        functools.partial(pack_small_kernel, parts, halves, first),
        in_specs=[vmem()] * 5 + [anywhere()],
        out_specs=[vmem()] * (parts + 1),
        out_shape=[jax.ShapeDtypeStruct((first[-2], lanes), bf16)] * parts
        + [jax.ShapeDtypeStruct((first[-1], lanes), bf16)],
        compiler_params=params(),
        name="pack_small",
    )(field, sdev, vert, loc, stat, after)


def spread_kernel(parts, halves, levels, first, after, *refs):
    messages, (wide_field, wide_sdev, left_end, right_end, loc, stat) = (
        refs[:parts],
        refs[parts:],
    )
    rows = wide_field.shape[1] // parts
    lanes = messages[0].shape[1]
    width = lanes // parts
    group = lane_groups((rows, lanes), width)
    ends = (left_end, right_end)
    for s, message in enumerate(messages):
        x = message[:rows, :].astype(f32) + message[rows : 2 * rows, :].astype(f32)
        for h in range(halves):
            wide = []
            for t in range(2):
                one = jnp.where(group == 2 * h + t, x, 0.0)
                both = one
                for k in range(1, parts):
                    both = both + pltpu.roll(one, k * width, 1)
                wide.append(both)
            wide_field[h, s * rows : (s + 1) * rows, :] = wide[0]
            wide_sdev[h, s * rows : (s + 1) * rows, :] = wide[1]
            ends[h][0, s * rows : (s + 1) * rows, :] = (wide[0] * wide[1]).astype(bf16)
    for begin, out in ((first[2], loc), (first[3], stat)):
        out[...] = jnp.concatenate(
            [m[begin : begin + ceil_to(levels, 16), :].astype(f32)[:levels] for m in messages],
            axis=0,
        ).astype(bf16)


def spread(messages, levels, rows, slots, parts, halves, after):
    lanes = messages[0].shape[1]
    first = message_rows(levels, rows, slots, lanes)
    wide = jax.ShapeDtypeStruct((halves, parts * rows, lanes), f32)
    end = jax.ShapeDtypeStruct((1, parts * rows, lanes), bf16)
    matrix = jax.ShapeDtypeStruct((parts * levels, lanes), bf16)
    return pl.pallas_call(
        functools.partial(spread_kernel, parts, halves, levels, first),
        in_specs=[anywhere()] + [vmem()] * parts,
        out_specs=[vmem()] * 6,
        out_shape=[wide, wide, end, end, matrix, matrix],
        compiler_params=params(),
        name="spread",
    )(after, *messages)


def product_kernel(parts, field_ref, *refs):
    xs, ends = refs[:parts], refs[-2:]
    count, _, rows, _ = xs[0].shape
    for s, x in enumerate(xs):
        here = slice(s * rows, (s + 1) * rows)
        for h, end in enumerate(ends):
            scale = field_ref[h, here, :]
            for k in range(count):
                end[k, here, :] = (x[k, h].astype(f32) * scale).astype(bf16)


def product(wide_field, xs, after):
    parts = len(xs)
    count, halves, rows, lanes = xs[0].shape
    step = 2 if count % 2 == 0 else 1
    end = jax.ShapeDtypeStruct((count, parts * rows, lanes), bf16)
    return pl.pallas_call(
        functools.partial(product_kernel, parts),
        grid=(count // step,),
        in_specs=[pl.BlockSpec(wide_field.shape, lambda i: (0, 0, 0))]
        + [pl.BlockSpec((step, halves, rows, lanes), lambda i: (i, 0, 0, 0))] * parts
        + [anywhere()] * len(after),
        out_specs=[pl.BlockSpec((step, parts * rows, lanes), lambda i: (i, 0, 0))] * halves,
        out_shape=[end] * halves,
        cost_estimate=cost(count * 1e6, count * halves * parts * rows * lanes * 4),
        compiler_params=params(count),
        name="product",
    )(wide_field, *xs, *after)


def filter_kernel(pair, has_total, matrix_ref, left, first, last, right, *refs):
    refs = list(refs)
    stack = refs.pop()
    total_out = refs.pop()
    total_in = refs.pop() if has_total else None
    xs = refs
    rows, lanes = first.shape[1:]

    @pl.when(pl.program_id(0) == 0)
    def _():
        if has_total:
            total_out[...] = total_in[...]
        else:
            total_out[...] = jnp.zeros_like(total_out)

    for n, ref in enumerate((left, first, last, right)):
        for k in range(pair):
            stack[n * rows : (n + 1) * rows, k * lanes : (k + 1) * lanes] = ref[k]
    for h in range(total_out.shape[0]):
        y = jnp.dot(
            matrix_ref[...], stack[h * rows : (h + 3) * rows, :], preferred_element_type=f32
        )
        piece = rows // len(xs)
        for s, x in enumerate(xs):
            here = slice(s * piece, (s + 1) * piece)
            add = total_out[h, here, :]
            for k in range(pair):
                add = add + x[k, h].astype(f32) * y[here, k * lanes : (k + 1) * lanes]
            total_out[h, here, :] = add


def filtered(matrix, left, first, last, right, xs, total):
    count, rows, lanes = first.shape
    pair = 2 if count % 2 == 0 else 1
    halves = 2
    piece = rows // len(xs)
    edge = pl.BlockSpec((pair, rows, lanes), lambda i: (i, 0, 0))
    whole = pl.BlockSpec((halves, rows, lanes), lambda i: (0, 0, 0))
    return pl.pallas_call(
        functools.partial(filter_kernel, pair, total is not None),
        grid=(count // pair,),
        in_specs=[pl.BlockSpec(matrix.shape, lambda i: (0, 0))]
        + [edge] * 4
        + [pl.BlockSpec((pair, halves, piece, lanes), lambda i: (i, 0, 0, 0))] * len(xs)
        + ([whole] if total is not None else []),
        out_specs=whole,
        out_shape=jax.ShapeDtypeStruct((halves, rows, lanes), f32),
        scratch_shapes=[pltpu.VMEM((4 * rows, pair * lanes), bf16)],
        cost_estimate=cost(
            2 * halves * matrix.shape[0] * matrix.shape[1] * lanes * count,
            count * rows * lanes * 12,
        ),
        compiler_params=params(count),
        name="filtered",
    )(matrix, left, first, last, right, *xs, *([total] if total is not None else []))


def fold_kernel(parts, block_rows, total_ref, static_ref, blocks_ref, mixed):
    halves, rows, lanes = total_ref.shape
    width = lanes // parts
    levels = rows // block_lon
    for h in range(halves):
        x = ens_weight * total_ref[h] + (static_weight / parts) * static_ref[h]
        folded = x
        for k in range(1, parts):
            folded = folded + pltpu.roll(x, k * width, 1)
        mixed[h * rows : (h + 1) * rows, :] = folded
    group = lane_groups((levels, lanes), block_lat)
    for h in range(halves):
        strips = [mixed[pl.ds(h * rows + i, levels, stride=block_lon), :] for i in range(block_lon)]
        for b in range(block_rows):
            out = None
            for i, strip in enumerate(strips):
                moved = pltpu.roll(strip, ((i - b) * block_lat) % lanes, 1)
                out = moved if out is None else jnp.where(group == i, moved, out)
            blocks_ref[b, h * levels : (h + 1) * levels, :] = out


def fold(total, static, parts):
    halves, rows, lanes = total.shape
    levels = rows // block_lon
    block_rows = lanes // parts // block_lat
    return pl.pallas_call(
        functools.partial(fold_kernel, parts, block_rows),
        in_specs=[vmem()] * 2,
        out_specs=vmem(),
        out_shape=jax.ShapeDtypeStruct((block_rows, halves * levels, lanes), f32),
        scratch_shapes=[pltpu.VMEM((halves * rows, lanes), f32)],
        cost_estimate=cost(2e6, 2e6),
        compiler_params=params(),
        name="fold",
    )(total, static)


def split(x):
    high = x.astype(bf16)
    return high, (x - high.astype(f32)).astype(bf16)


def horiz_kernel(horiz_ref, high, low, high_t, low_t):
    hi, lo = split(horiz_ref[...])
    high[...] = hi
    low[...] = lo
    flipped_hi, flipped_lo = split(horiz_ref[...].T)
    high_t[...] = flipped_hi
    low_t[...] = flipped_lo


def horiz_parts(horiz):
    slots, cells = horiz.shape
    return pl.pallas_call(
        horiz_kernel,
        in_specs=[vmem()],
        out_specs=[vmem()] * 4,
        out_shape=[jax.ShapeDtypeStruct((slots, cells), bf16)] * 2
        + [jax.ShapeDtypeStruct((cells, slots), bf16)] * 2,
        cost_estimate=cost(1e6, 2e6),
        compiler_params=params(),
        name="horiz_parts",
    )(horiz)


def product3(a, high, low):
    a_high, a_low = split(a)
    dot = functools.partial(jnp.dot, preferred_element_type=f32)
    return dot(a_high, high) + (dot(a_low, high) + dot(a_high, low))


def observe_kernel(
    parts, halves, lat_blocks, blocks_ref, *refs
):
    verts, (
        high, low, high_t, low_t, ids_ref, value_ref, rinv_ref, share_ref, *outs, vert_ref
    ) = refs[:parts], refs[parts:]
    block_rows, stacked, cells = blocks_ref.shape
    levels = stacked // halves
    piece = levels // parts
    base = lax.axis_index("lev") * block_rows
    ids = ids_ref[...]
    for s, ref in enumerate(verts):
        rows = ref[...].astype(f32)
        for t in range(rows.shape[0] // piece):
            vert_ref[s * piece : (s + 1) * piece, t * cells : (t + 1) * cells] = rows[
                t * piece : (t + 1) * piece
            ]
    vert = vert_ref[...]
    picks = [
        [ids == h * lat_blocks + base + b for b in range(block_rows)] for h in range(halves)
    ]
    mine = None
    hx = jnp.zeros(ids.shape, f32)
    for b in range(block_rows):
        projected = product3(blocks_ref[b], high_t[...], low_t[...])
        for h in range(halves):
            one = jnp.sum(projected[h * levels : (h + 1) * levels] * vert, axis=0, keepdims=True)
            hx = jnp.where(picks[h][b], one, hx)
            mine = picks[h][b] if mine is None else mine | picks[h][b]
    miss = hx - value_ref[...]
    dep = jnp.where(mine, rinv_ref[...] * miss, 0.0)
    total = 0.5 * jnp.sum(dep * miss, axis=1, keepdims=True)
    slot = lax.axis_index("lon") * parts + lax.axis_index("lev")
    spot = lax.broadcasted_iota(jnp.int32, share_ref.shape, 0) * cells
    spot = spot + lax.broadcasted_iota(jnp.int32, share_ref.shape, 1)
    share_ref[...] = jnp.where(spot == slot, jnp.broadcast_to(total, share_ref.shape), 0.0)
    both = [[], []]
    for b in range(block_rows):
        weights = jnp.concatenate(
            [vert * jnp.where(picks[h][b], dep, 0.0) for h in range(halves)], axis=0
        )
        adjoint = product3(weights, high[...], low[...])
        both[0].append(blocks_ref[b])
        both[1].append(adjoint)
    for s, ref in enumerate(outs):
        pieces = [
            x[h * levels + s * piece : h * levels + (s + 1) * piece]
            for b in range(block_rows)
            for x in (both[0][b], both[1][b])
            for h in range(halves)
        ]
        ref[...] = jnp.concatenate(pieces, axis=0).astype(bf16)


def observe(blocks, verts, horiz, ids, value, rinv, parts, halves, lat_blocks):
    block_rows, stacked, cells = blocks.shape
    back = jax.ShapeDtypeStruct((2 * block_rows * stacked // parts, cells), bf16)
    share = jax.ShapeDtypeStruct((8, 128), f32)
    return pl.pallas_call(
        functools.partial(observe_kernel, parts, halves, lat_blocks),
        in_specs=[vmem()] * (8 + len(verts)),
        scratch_shapes=[pltpu.VMEM((stacked // halves, ids.shape[1]), f32)],
        out_specs=[vmem()] * (parts + 1),
        out_shape=[share] + [back] * parts,
        cost_estimate=cost(1e9, 4e6),
        compiler_params=params(),
        name="observe",
    )(blocks, *verts, *horiz, ids, value, rinv)


def unpack_kernel(halves, levels, *refs):
    *backs, increment_ref, adjoint_ref, strips = refs
    rows, lanes = backs[0].shape
    width = lanes // len(backs)
    block_rows = width // block_lat
    count = rows // block_rows
    group = lane_groups((count, lanes), block_lat)
    pieces = []
    for s, ref in enumerate(backs):
        x = ref[...].astype(f32)
        for b in range(block_rows):
            place = my_partner(s) * width + b * block_lat
            pieces.append((place, x[b * count : (b + 1) * count]))
    for i in range(block_lon):
        strip = None
        for place, x in pieces:
            x = jnp.where(group == i, x, 0.0)
            x = pltpu.roll(x, lax.rem(place + lanes - i * block_lat, lanes), 1)
            strip = x if strip is None else strip + x
        strips[i * count : (i + 1) * count, :] = strip
    for n, out_ref in enumerate((increment_ref, adjoint_ref)):
        for h in range(halves):
            for l in range(levels):
                row = (n * halves + h) * levels + l
                first = (l * halves + h) * block_lon
                out_ref[first : first + block_lon, :] = strips[
                    pl.ds(row, block_lon, stride=count), :
                ]


def unpack(backs, levels, columns, lanes):
    halves = columns // block_lon
    outs = pl.pallas_call(
        functools.partial(unpack_kernel, halves, levels),
        in_specs=[vmem()] * len(backs),
        out_specs=[vmem()] * 2,
        out_shape=[jax.ShapeDtypeStruct((levels * columns, lanes), f32)] * 2,
        scratch_shapes=[pltpu.VMEM((2 * levels * columns, lanes), f32)],
        cost_estimate=cost(1e7, 1e6),
        compiler_params=params(),
        name="unpack",
    )(*backs)
    return [x.reshape(levels, columns, lanes) for x in outs]


def exchange(blocks):
    count = lax.axis_size("lev")
    return [blocks[0]] + [
        lax.ppermute(blocks[place], "lev", [(i, i ^ place) for i in range(count)])
        for place in range(1, count)
    ]


def bands_kernel(rows, span, lon_ref, static_ref, *outs):
    for taper_ref, out in zip((lon_ref, static_ref), outs):
        column = lax.broadcasted_iota(jnp.int32, out.shape, 1)
        offset = column // span * rows + column % rows
        offset = offset - lax.broadcasted_iota(jnp.int32, out.shape, 0)
        band = jnp.zeros(out.shape, f32)
        for d in range(2 * rows + 1):
            band = jnp.where(offset == d, taper_ref[d], band)
        out[...] = band


def bands(lon_taper, static_taper, rows, span):
    shape = jax.ShapeDtypeStruct((rows, 3 * span), f32)
    return pl.pallas_call(
        functools.partial(bands_kernel, rows, span),
        in_specs=[smem()] * 2,
        out_specs=[vmem()] * 2,
        out_shape=[shape] * 2,
        compiler_params=params(),
        name="bands",
    )(lon_taper.astype(f32), static_taper.astype(f32))


def total_of(x, axis):
    reach = 1
    while reach < lax.axis_size(axis):
        pairs = [(i, i ^ reach) for i in range(lax.axis_size(axis))]
        x = x + lax.ppermute(x, axis, pairs)
        reach *= 2
    return x


def operator(vert_rows, band, parts, levels, rows):
    total = parts * levels
    span = total * rows
    column = jnp.arange(3 * span)
    source = column % span // rows
    owner = my_partner(source // levels)
    pick = (jnp.arange(vert_rows.shape[1])[:, None] == (owner * levels + source % levels)[None, :])
    wide = jnp.dot(vert_rows, pick.astype(bf16), preferred_element_type=f32).astype(bf16)
    grow = (jnp.arange(span)[:, None] // rows == jnp.arange(total)[None, :]).astype(bf16)
    tall = jnp.dot(grow, wide, preferred_element_type=f32)
    return (tall.reshape(total, rows, 3 * span) * band[None]).astype(bf16).reshape(span, 3 * span)


def filters_after(chunk, chunks):
    held = 2 if chunk >= chunks - 3 else 1
    last = chunks - 1 if chunk == chunks - 1 else chunk - held
    held = 2 if chunk - 1 >= chunks - 3 else 1
    return range(max(chunk - 1 - held + 1, 0), last + 1)


def chunk_sizes(groups):
    ends = [groups * sum(plan[: n + 1]) // sum(plan) for n in range(len(plan))]
    return [end - begin for begin, end in zip([0] + ends, ends)]


def body(
    field,
    ens,
    sdev,
    lon_taper,
    static_taper,
    loc_vert,
    static_vert,
    obs_block,
    obs_value,
    obs_rinv,
    obs_horiz,
    obs_vert,
):
    members, levels, columns, lanes = ens.shape
    parts = lax.axis_size("lev")
    rows = lon_taper.shape[0] // 2
    halves = columns // rows
    lat_blocks = lanes // block_lat
    slots = obs_block.shape[0]

    sizes = chunk_sizes(members // parts)
    starts = [sum(sizes[:n]) for n in range(len(sizes))]
    first_pack = pack(ens, starts[0], sizes[0], parts, halves, lon_taper)
    *messages, vert_rows = pack_small(
        field, sdev, obs_vert, loc_vert, static_vert, parts, halves, first_pack[0]
    )
    half_rows = levels * rows
    received = [exchange(first_pack)]
    after = messages[0]
    messages = exchange(messages)
    for n in range(1, len(sizes)):
        packed = pack(ens, starts[n], sizes[n], parts, halves, after)
        after = packed[0]
        received.append(exchange(packed))

    verts = exchange([vert_rows] * parts)
    wide_field, wide_sdev, static_first, static_last, loc_all, stat_all = spread(
        messages, levels, half_rows, slots, parts, halves, after
    )
    lon_band, static_band = bands(lon_taper, static_taper, rows, parts * half_rows)
    loc_matrix = operator(loc_all, lon_band, parts, levels, rows)
    stat_matrix = operator(stat_all, static_band, parts, levels, rows)
    horiz = horiz_parts(obs_horiz)

    def halo(first, last):
        left = lax.ppermute(last, "lon", shift_by("lon", 1))
        right = lax.ppermute(first, "lon", shift_by("lon", -1))
        return left, right

    left, right = halo(static_first, static_last)
    static = filtered(stat_matrix, left, static_first, static_last, right, [wide_sdev[None]], None)
    total = None
    ready = []
    after = [static_first]
    for n, xs in enumerate(received):
        first, last = product(wide_field, xs, after)
        left, right = halo(first, last)
        ready.append((left, first, last, right, xs))
        after = [first] if n else [first, static]
        for m in filters_after(n, len(received)):
            total = filtered(loc_matrix, *ready[m], total)
            after = [total]

    blocks = fold(total, static, parts)

    nblk = columns // block_lon * lat_blocks
    ids = jnp.where(obs_block >= 0, obs_block - lax.axis_index("lon") * nblk, -1)
    share, *backs = observe(
        blocks, verts, horiz, ids[None], obs_value[None], obs_rinv[None],
        parts, halves, lat_blocks,
    )
    backs = exchange(backs)
    shares = total_of(total_of(share, "lon"), "lev")
    obs_cost = jnp.sum(shares)

    increment, adjoint_field = unpack(backs, levels, columns, lanes)
    return (increment, adjoint_field, obs_cost)


def solution(mesh):
    return jax.shard_map(
        body,
        mesh=mesh,
        in_specs=(
            P("lev", "lon", None),
            P(None, "lev", "lon", None),
            P("lev", "lon", None),
            P(),
            P(),
            P("lev", None),
            P("lev", None),
            P("lon"),
            P("lon"),
            P("lon"),
            P("lon", None),
            P("lon", "lev"),
        ),
        out_specs=(P("lev", "lon", None), P("lev", "lon", None), P()),
        check_vma=False,
    )
```

```python
import functools

import jax
import jax.numpy as jnp
from jax import lax
from jax.experimental import pallas as pl
from jax.experimental.pallas import tpu as pltpu
from jax.sharding import PartitionSpec as P


ens_weight = 0.8
static_weight = 0.5
block_lon = 8
block_lat = 16
LIMIT = 44
plan = (2, 4, 4, 4, 2, 2, 2)
f32 = jnp.float32
bf16 = jnp.bfloat16


def my_partner(place):
    return lax.axis_index("lev") ^ place


def shift_by(axis, amount):
    count = lax.axis_size(axis)
    return [(i, (i + amount) % count) for i in range(count)]


def vmem():
    return pl.BlockSpec(memory_space=pltpu.VMEM)


def anywhere():
    return pl.BlockSpec(memory_space=pl.ANY)


def params(count=0):
    return pltpu.CompilerParams(vmem_limit_bytes=(58 if count > 20 else LIMIT) * 2**20)


def smem():
    return pl.BlockSpec(memory_space=pltpu.SMEM)


def cost(flops, nbytes):
    return pl.CostEstimate(flops=int(flops), bytes_accessed=int(nbytes), transcendentals=0)


def lane_groups(shape, width):
    return lax.broadcasted_iota(jnp.int32, shape, len(shape) - 1) // width


def regroup(sources, quarter, parts, width):
    group = lane_groups(sources[0].shape, width)
    out = None
    for p, source in enumerate(sources):
        turn = lax.rem(p - quarter + parts, parts) * width
        moved = pltpu.roll(source, turn, source.ndim - 1)
        out = moved if out is None else jnp.where(group == p, moved, out)
    return out


def pack_kernel(parts, halves, ens_ref, after, *outs):
    levels, columns, lanes = ens_ref.shape[1:]
    width = lanes // parts
    rows = columns // halves
    sources = [ens_ref[p].astype(f32).reshape(levels * columns, lanes) for p in range(parts)]
    for s, out in enumerate(outs):
        packed = regroup(sources, my_partner(s), parts, width)
        packed = packed.reshape(levels, halves, rows, lanes)
        for h in range(halves):
            out[0, h] = packed[:, h].reshape(levels * rows, lanes).astype(bf16)


def pack(ens, start, count, parts, halves, after):
    _, levels, columns, lanes = ens.shape
    rows = levels * columns // halves
    shape = jax.ShapeDtypeStruct((count, halves, rows, lanes), bf16)
    return pl.pallas_call(
        functools.partial(pack_kernel, parts, halves),
        grid=(count,),
        in_specs=[
            pl.BlockSpec((parts, levels, columns, lanes), lambda i: (start + i, 0, 0, 0)),
            anywhere(),
        ],
        out_specs=[pl.BlockSpec((1, halves, rows, lanes), lambda i: (i, 0, 0, 0))] * parts,
        out_shape=[shape] * parts,
        cost_estimate=cost(count * 4e6, count * parts * halves * rows * lanes * 4),
        compiler_params=params(99),
        name="pack",
    )(ens, after)


def ceil_to(x, unit):
    return -(-x // unit) * unit


def message_rows(levels, half_rows, slots, lanes):
    loc = 2 * half_rows
    stat = loc + ceil_to(levels, 16)
    return 0, half_rows, loc, stat, stat + ceil_to(levels, 16), levels * slots // lanes


def pack_small_kernel(
    parts, halves, first, field_ref, sdev_ref, vert_ref, loc_ref, stat_ref, after, *outs
):
    *outs, flat_ref = outs
    levels, columns, lanes = field_ref.shape
    width = lanes // parts
    rows = columns // halves
    slots = vert_ref.shape[0]
    sources = []
    for h in range(halves):
        for ref in (field_ref, sdev_ref):
            sources.append(ref[:, h * rows : (h + 1) * rows, :].reshape(levels * rows, lanes))
    flat = vert_ref[...].T
    flat_ref[...] = jnp.concatenate(
        [flat[:, t : t + lanes] for t in range(0, slots, lanes)], axis=0
    ).astype(bf16)
    for s, out in enumerate(outs):
        high, low = split(regroup(sources, my_partner(s), parts, width))
        out[first[0] : first[1], :] = high
        out[first[1] : first[2], :] = low
        for begin, ref in ((first[2], loc_ref), (first[3], stat_ref)):
            out[begin : begin + ceil_to(levels, 16), :] = jnp.zeros(
                (ceil_to(levels, 16), lanes), bf16
            )
            out[begin : begin + levels, : ref.shape[1]] = ref[...]


def pack_small(field, sdev, vert, loc, stat, parts, halves, after):
    levels, columns, lanes = field.shape
    first = message_rows(levels, levels * columns // halves, vert.shape[0], lanes)
    return pl.pallas_call(
        functools.partial(pack_small_kernel, parts, halves, first),
        in_specs=[vmem()] * 5 + [anywhere()],
        out_specs=[vmem()] * (parts + 1),
        out_shape=[jax.ShapeDtypeStruct((first[-2], lanes), bf16)] * parts
        + [jax.ShapeDtypeStruct((first[-1], lanes), bf16)],
        compiler_params=params(),
        name="pack_small",
    )(field, sdev, vert, loc, stat, after)


def spread_kernel(parts, halves, levels, first, after, *refs):
    messages, (wide_field, wide_sdev, left_end, right_end, loc, stat) = (
        refs[:parts],
        refs[parts:],
    )
    rows = wide_field.shape[1] // parts
    lanes = messages[0].shape[1]
    width = lanes // parts
    group = lane_groups((rows, lanes), width)
    ends = (left_end, right_end)
    for s, message in enumerate(messages):
        x = message[:rows, :].astype(f32) + message[rows : 2 * rows, :].astype(f32)
        for h in range(halves):
            wide = []
            for t in range(2):
                one = jnp.where(group == 2 * h + t, x, 0.0)
                both = one
                for k in range(1, parts):
                    both = both + pltpu.roll(one, k * width, 1)
                wide.append(both)
            wide_field[h, s * rows : (s + 1) * rows, :] = wide[0]
            wide_sdev[h, s * rows : (s + 1) * rows, :] = wide[1]
            ends[h][0, s * rows : (s + 1) * rows, :] = (wide[0] * wide[1]).astype(bf16)
    for begin, out in ((first[2], loc), (first[3], stat)):
        out[...] = jnp.concatenate(
            [m[begin : begin + ceil_to(levels, 16), :].astype(f32)[:levels] for m in messages],
            axis=0,
        ).astype(bf16)


def spread(messages, levels, rows, slots, parts, halves, after):
    lanes = messages[0].shape[1]
    first = message_rows(levels, rows, slots, lanes)
    wide = jax.ShapeDtypeStruct((halves, parts * rows, lanes), f32)
    end = jax.ShapeDtypeStruct((1, parts * rows, lanes), bf16)
    matrix = jax.ShapeDtypeStruct((parts * levels, lanes), bf16)
    return pl.pallas_call(
        functools.partial(spread_kernel, parts, halves, levels, first),
        in_specs=[anywhere()] + [vmem()] * parts,
        out_specs=[vmem()] * 6,
        out_shape=[wide, wide, end, end, matrix, matrix],
        compiler_params=params(),
        name="spread",
    )(after, *messages)


def product_kernel(parts, field_ref, *refs):
    xs, ends = refs[:parts], refs[-2:]
    count, _, rows, _ = xs[0].shape
    for s, x in enumerate(xs):
        here = slice(s * rows, (s + 1) * rows)
        for h, end in enumerate(ends):
            scale = field_ref[h, here, :]
            for k in range(count):
                end[k, here, :] = (x[k, h].astype(f32) * scale).astype(bf16)


def product(wide_field, xs, after):
    parts = len(xs)
    count, halves, rows, lanes = xs[0].shape
    step = 2 if count % 2 == 0 else 1
    end = jax.ShapeDtypeStruct((count, parts * rows, lanes), bf16)
    return pl.pallas_call(
        functools.partial(product_kernel, parts),
        grid=(count // step,),
        in_specs=[pl.BlockSpec(wide_field.shape, lambda i: (0, 0, 0))]
        + [pl.BlockSpec((step, halves, rows, lanes), lambda i: (i, 0, 0, 0))] * parts
        + [anywhere()] * len(after),
        out_specs=[pl.BlockSpec((step, parts * rows, lanes), lambda i: (i, 0, 0))] * halves,
        out_shape=[end] * halves,
        cost_estimate=cost(count * 1e6, count * halves * parts * rows * lanes * 4),
        compiler_params=params(count),
        name="product",
    )(wide_field, *xs, *after)


def filter_kernel(pair, has_total, matrix_ref, left, first, last, right, *refs):
    refs = list(refs)
    stack = refs.pop()
    total_out = refs.pop()
    total_in = refs.pop() if has_total else None
    xs = refs
    rows, lanes = first.shape[1:]

    @pl.when(pl.program_id(0) == 0)
    def _():
        if has_total:
            total_out[...] = total_in[...]
        else:
            total_out[...] = jnp.zeros_like(total_out)

    for n, ref in enumerate((left, first, last, right)):
        for k in range(pair):
            stack[n * rows : (n + 1) * rows, k * lanes : (k + 1) * lanes] = ref[k]
    for h in range(total_out.shape[0]):
        y = jnp.dot(
            matrix_ref[...], stack[h * rows : (h + 3) * rows, :], preferred_element_type=f32
        )
        piece = rows // len(xs)
        for s, x in enumerate(xs):
            here = slice(s * piece, (s + 1) * piece)
            add = total_out[h, here, :]
            for k in range(pair):
                add = add + x[k, h].astype(f32) * y[here, k * lanes : (k + 1) * lanes]
            total_out[h, here, :] = add


def filtered(matrix, left, first, last, right, xs, total):
    count, rows, lanes = first.shape
    pair = 2 if count % 2 == 0 else 1
    halves = 2
    piece = rows // len(xs)
    edge = pl.BlockSpec((pair, rows, lanes), lambda i: (i, 0, 0))
    whole = pl.BlockSpec((halves, rows, lanes), lambda i: (0, 0, 0))
    return pl.pallas_call(
        functools.partial(filter_kernel, pair, total is not None),
        grid=(count // pair,),
        in_specs=[pl.BlockSpec(matrix.shape, lambda i: (0, 0))]
        + [edge] * 4
        + [pl.BlockSpec((pair, halves, piece, lanes), lambda i: (i, 0, 0, 0))] * len(xs)
        + ([whole] if total is not None else []),
        out_specs=whole,
        out_shape=jax.ShapeDtypeStruct((halves, rows, lanes), f32),
        scratch_shapes=[pltpu.VMEM((4 * rows, pair * lanes), bf16)],
        cost_estimate=cost(
            2 * halves * matrix.shape[0] * matrix.shape[1] * lanes * count,
            count * rows * lanes * 12,
        ),
        compiler_params=params(count),
        name="filtered",
    )(matrix, left, first, last, right, *xs, *([total] if total is not None else []))


def fold_kernel(parts, block_rows, total_ref, static_ref, blocks_ref, mixed):
    halves, rows, lanes = total_ref.shape
    width = lanes // parts
    levels = rows // block_lon
    for h in range(halves):
        x = ens_weight * total_ref[h] + (static_weight / parts) * static_ref[h]
        folded = x
        for k in range(1, parts):
            folded = folded + pltpu.roll(x, k * width, 1)
        mixed[h * rows : (h + 1) * rows, :] = folded
    group = lane_groups((levels, lanes), block_lat)
    for h in range(halves):
        strips = [mixed[pl.ds(h * rows + i, levels, stride=block_lon), :] for i in range(block_lon)]
        for b in range(block_rows):
            out = None
            for i, strip in enumerate(strips):
                moved = pltpu.roll(strip, ((i - b) * block_lat) % lanes, 1)
                out = moved if out is None else jnp.where(group == i, moved, out)
            blocks_ref[b, h * levels : (h + 1) * levels, :] = out


def fold(total, static, parts):
    halves, rows, lanes = total.shape
    levels = rows // block_lon
    block_rows = lanes // parts // block_lat
    return pl.pallas_call(
        functools.partial(fold_kernel, parts, block_rows),
        in_specs=[vmem()] * 2,
        out_specs=vmem(),
        out_shape=jax.ShapeDtypeStruct((block_rows, halves * levels, lanes), f32),
        scratch_shapes=[pltpu.VMEM((halves * rows, lanes), f32)],
        cost_estimate=cost(2e6, 2e6),
        compiler_params=params(),
        name="fold",
    )(total, static)


def split(x):
    high = x.astype(bf16)
    return high, (x - high.astype(f32)).astype(bf16)


def horiz_kernel(horiz_ref, high, low, high_t, low_t):
    hi, lo = split(horiz_ref[...])
    high[...] = hi
    low[...] = lo
    flipped_hi, flipped_lo = split(horiz_ref[...].T)
    high_t[...] = flipped_hi
    low_t[...] = flipped_lo


def horiz_parts(horiz):
    slots, cells = horiz.shape
    return pl.pallas_call(
        horiz_kernel,
        in_specs=[vmem()],
        out_specs=[vmem()] * 4,
        out_shape=[jax.ShapeDtypeStruct((slots, cells), bf16)] * 2
        + [jax.ShapeDtypeStruct((cells, slots), bf16)] * 2,
        cost_estimate=cost(1e6, 2e6),
        compiler_params=params(),
        name="horiz_parts",
    )(horiz)


def product3(a, high, low):
    a_high, a_low = split(a)
    dot = functools.partial(jnp.dot, preferred_element_type=f32)
    return dot(a_high, high) + (dot(a_low, high) + dot(a_high, low))


def vert_kernel(*refs):
    *verts, out = refs
    lanes = verts[0].shape[1]
    piece = out.shape[0] // len(verts)
    for s, ref in enumerate(verts):
        rows = ref[...].astype(f32)
        for t in range(out.shape[1] // lanes):
            here = slice(t * piece, (t + 1) * piece)
            out[s * piece : (s + 1) * piece, t * lanes : (t + 1) * lanes] = rows[here]


def join_vert(verts, levels, slots):
    return pl.pallas_call(
        vert_kernel,
        in_specs=[vmem()] * len(verts),
        out_specs=vmem(),
        out_shape=jax.ShapeDtypeStruct((len(verts) * levels, slots), f32),
        cost_estimate=cost(1e6, 1e6),
        compiler_params=params(),
        name="join_vert",
    )(*verts)


def block_picks(ids, halves, block_rows, lat_blocks):
    base = lax.axis_index("lev") * block_rows
    return [[ids == h * lat_blocks + base + b for b in range(block_rows)] for h in range(halves)]


def depart_kernel(
    halves, lat_blocks, blocks_ref, vert_ref, high_t, low_t, ids_ref, value_ref, rinv_ref,
    dep_ref, share_ref
):
    block_rows, stacked, cells = blocks_ref.shape
    levels = stacked // halves
    vert = vert_ref[...]
    picks = block_picks(ids_ref[...], halves, block_rows, lat_blocks)
    mine = None
    hx = jnp.zeros(ids_ref.shape, f32)
    for b in range(block_rows):
        projected = product3(blocks_ref[b], high_t[...], low_t[...])
        for h in range(halves):
            one = jnp.sum(projected[h * levels : (h + 1) * levels] * vert, axis=0, keepdims=True)
            hx = jnp.where(picks[h][b], one, hx)
            mine = picks[h][b] if mine is None else mine | picks[h][b]
    miss = hx - value_ref[...]
    dep = jnp.where(mine, rinv_ref[...] * miss, 0.0)
    dep_ref[...] = dep
    total = 0.5 * jnp.sum(dep * miss, axis=1, keepdims=True)
    slot = lax.axis_index("lon") * lax.axis_size("lev") + lax.axis_index("lev")
    spot = lax.broadcasted_iota(jnp.int32, share_ref.shape, 0) * cells
    spot = spot + lax.broadcasted_iota(jnp.int32, share_ref.shape, 1)
    share_ref[...] = jnp.where(spot == slot, jnp.broadcast_to(total, share_ref.shape), 0.0)


def adjoint_kernel(
    parts, halves, lat_blocks, blocks_ref, vert_ref, high, low, ids_ref, dep_ref, *outs
):
    block_rows, stacked, _ = blocks_ref.shape
    levels = stacked // halves
    piece = levels // parts
    vert = vert_ref[...]
    dep = dep_ref[...]
    picks = block_picks(ids_ref[...], halves, block_rows, lat_blocks)
    both = [[], []]
    for b in range(block_rows):
        weights = jnp.concatenate(
            [vert * jnp.where(picks[h][b], dep, 0.0) for h in range(halves)], axis=0
        )
        both[0].append(blocks_ref[b])
        both[1].append(product3(weights, high[...], low[...]))
    for s, ref in enumerate(outs):
        pieces = [
            x[h * levels + s * piece : h * levels + (s + 1) * piece]
            for b in range(block_rows)
            for x in (both[0][b], both[1][b])
            for h in range(halves)
        ]
        ref[...] = jnp.concatenate(pieces, axis=0).astype(bf16)


def observe(blocks, vert, horiz, ids, value, rinv, parts, halves, lat_blocks):
    high, low, high_t, low_t = horiz
    block_rows, stacked, cells = blocks.shape
    dep, share = pl.pallas_call(
        functools.partial(depart_kernel, halves, lat_blocks),
        in_specs=[vmem()] * 7,
        out_specs=[vmem()] * 2,
        out_shape=[
            jax.ShapeDtypeStruct(ids.shape, f32),
            jax.ShapeDtypeStruct((8, cells), f32),
        ],
        cost_estimate=cost(1e9, 4e6),
        compiler_params=params(),
        name="depart",
    )(blocks, vert, high_t, low_t, ids, value, rinv)
    back = jax.ShapeDtypeStruct((2 * block_rows * stacked // parts, cells), bf16)
    backs = pl.pallas_call(
        functools.partial(adjoint_kernel, parts, halves, lat_blocks),
        in_specs=[vmem()] * 6,
        out_specs=[vmem()] * parts,
        out_shape=[back] * parts,
        cost_estimate=cost(1e9, 4e6),
        compiler_params=params(),
        name="adjoint",
    )(blocks, vert, high, low, ids, dep)
    return share, backs


def unpack_kernel(halves, levels, *refs):
    *backs, increment_ref, adjoint_ref, strips = refs
    rows, lanes = backs[0].shape
    width = lanes // len(backs)
    block_rows = width // block_lat
    count = rows // block_rows
    group = lane_groups((count, lanes), block_lat)
    pieces = []
    for s, ref in enumerate(backs):
        x = ref[...].astype(f32)
        for b in range(block_rows):
            place = my_partner(s) * width + b * block_lat
            pieces.append((place, x[b * count : (b + 1) * count]))
    for i in range(block_lon):
        strip = None
        for place, x in pieces:
            x = jnp.where(group == i, x, 0.0)
            x = pltpu.roll(x, lax.rem(place + lanes - i * block_lat, lanes), 1)
            strip = x if strip is None else strip + x
        strips[i * count : (i + 1) * count, :] = strip
    for n, out_ref in enumerate((increment_ref, adjoint_ref)):
        for h in range(halves):
            for l in range(levels):
                row = (n * halves + h) * levels + l
                first = (l * halves + h) * block_lon
                out_ref[first : first + block_lon, :] = strips[
                    pl.ds(row, block_lon, stride=count), :
                ]


def unpack(backs, levels, columns, lanes):
    halves = columns // block_lon
    outs = pl.pallas_call(
        functools.partial(unpack_kernel, halves, levels),
        in_specs=[vmem()] * len(backs),
        out_specs=[vmem()] * 2,
        out_shape=[jax.ShapeDtypeStruct((levels * columns, lanes), f32)] * 2,
        scratch_shapes=[pltpu.VMEM((2 * levels * columns, lanes), f32)],
        cost_estimate=cost(1e7, 1e6),
        compiler_params=params(),
        name="unpack",
    )(*backs)
    return [x.reshape(levels, columns, lanes) for x in outs]


def exchange(blocks):
    count = lax.axis_size("lev")
    return [blocks[0]] + [
        lax.ppermute(blocks[place], "lev", [(i, i ^ place) for i in range(count)])
        for place in range(1, count)
    ]


def bands_kernel(rows, span, lon_ref, static_ref, *outs):
    for taper_ref, out in zip((lon_ref, static_ref), outs):
        column = lax.broadcasted_iota(jnp.int32, out.shape, 1)
        offset = column // span * rows + column % rows
        offset = offset - lax.broadcasted_iota(jnp.int32, out.shape, 0)
        band = jnp.zeros(out.shape, f32)
        for d in range(2 * rows + 1):
            band = jnp.where(offset == d, taper_ref[d], band)
        out[...] = band


def bands(lon_taper, static_taper, rows, span):
    shape = jax.ShapeDtypeStruct((rows, 3 * span), f32)
    return pl.pallas_call(
        functools.partial(bands_kernel, rows, span),
        in_specs=[smem()] * 2,
        out_specs=[vmem()] * 2,
        out_shape=[shape] * 2,
        compiler_params=params(),
        name="bands",
    )(lon_taper.astype(f32), static_taper.astype(f32))


def total_of(x, axis):
    reach = 1
    while reach < lax.axis_size(axis):
        pairs = [(i, i ^ reach) for i in range(lax.axis_size(axis))]
        x = x + lax.ppermute(x, axis, pairs)
        reach *= 2
    return x


def operator(vert_rows, band, parts, levels, rows):
    total = parts * levels
    span = total * rows
    column = jnp.arange(3 * span)
    source = column % span // rows
    owner = my_partner(source // levels)
    pick = (jnp.arange(vert_rows.shape[1])[:, None] == (owner * levels + source % levels)[None, :])
    wide = jnp.dot(vert_rows, pick.astype(bf16), preferred_element_type=f32).astype(bf16)
    grow = (jnp.arange(span)[:, None] // rows == jnp.arange(total)[None, :]).astype(bf16)
    tall = jnp.dot(grow, wide, preferred_element_type=f32)
    return (tall.reshape(total, rows, 3 * span) * band[None]).astype(bf16).reshape(span, 3 * span)


def filters_after(chunk, chunks):
    held = 2 if chunk >= chunks - 3 else 1
    last = chunks - 1 if chunk == chunks - 1 else chunk - held
    held = 2 if chunk - 1 >= chunks - 3 else 1
    return range(max(chunk - 1 - held + 1, 0), last + 1)


def chunk_sizes(groups):
    ends = [groups * sum(plan[: n + 1]) // sum(plan) for n in range(len(plan))]
    return [end - begin for begin, end in zip([0] + ends, ends)]


def body(
    field,
    ens,
    sdev,
    lon_taper,
    static_taper,
    loc_vert,
    static_vert,
    obs_block,
    obs_value,
    obs_rinv,
    obs_horiz,
    obs_vert,
):
    members, levels, columns, lanes = ens.shape
    parts = lax.axis_size("lev")
    rows = lon_taper.shape[0] // 2
    halves = columns // rows
    lat_blocks = lanes // block_lat
    slots = obs_block.shape[0]

    sizes = chunk_sizes(members // parts)
    starts = [sum(sizes[:n]) for n in range(len(sizes))]
    first_pack = pack(ens, starts[0], sizes[0], parts, halves, lon_taper)
    *messages, vert_rows = pack_small(
        field, sdev, obs_vert, loc_vert, static_vert, parts, halves, first_pack[0]
    )
    half_rows = levels * rows
    received = [exchange(first_pack)]
    after = messages[0]
    messages = exchange(messages)
    for n in range(1, len(sizes)):
        packed = pack(ens, starts[n], sizes[n], parts, halves, after)
        after = packed[0]
        received.append(exchange(packed))

    verts = exchange([vert_rows] * parts)
    wide_field, wide_sdev, static_first, static_last, loc_all, stat_all = spread(
        messages, levels, half_rows, slots, parts, halves, after
    )
    lon_band, static_band = bands(lon_taper, static_taper, rows, parts * half_rows)
    loc_matrix = operator(loc_all, lon_band, parts, levels, rows)
    stat_matrix = operator(stat_all, static_band, parts, levels, rows)
    horiz = horiz_parts(obs_horiz)

    def halo(first, last):
        left = lax.ppermute(last, "lon", shift_by("lon", 1))
        right = lax.ppermute(first, "lon", shift_by("lon", -1))
        return left, right

    left, right = halo(static_first, static_last)
    static = filtered(stat_matrix, left, static_first, static_last, right, [wide_sdev[None]], None)
    total = None
    ready = []
    after = [static_first]
    for n, xs in enumerate(received):
        first, last = product(wide_field, xs, after)
        left, right = halo(first, last)
        ready.append((left, first, last, right, xs))
        after = [first] if n else [first, static]
        for m in filters_after(n, len(received)):
            total = filtered(loc_matrix, *ready[m], total)
            after = [total]

    blocks = fold(total, static, parts)

    nblk = columns // block_lon * lat_blocks
    ids = jnp.where(obs_block >= 0, obs_block - lax.axis_index("lon") * nblk, -1)
    share, backs = observe(
        blocks, join_vert(verts, levels, slots), horiz, ids[None], obs_value[None], obs_rinv[None],
        parts, halves, lat_blocks,
    )
    backs = exchange(backs)
    shares = total_of(total_of(share, "lon"), "lev")
    obs_cost = jnp.sum(shares)

    increment, adjoint_field = unpack(backs, levels, columns, lanes)
    return (increment, adjoint_field, obs_cost)


def solution(mesh):
    return jax.shard_map(
        body,
        mesh=mesh,
        in_specs=(
            P("lev", "lon", None),
            P(None, "lev", "lon", None),
            P("lev", "lon", None),
            P(),
            P(),
            P("lev", None),
            P("lev", None),
            P("lon"),
            P("lon"),
            P("lon"),
            P("lon", None),
            P("lon", "lev"),
        ),
        out_specs=(P("lev", "lon", None), P("lev", "lon", None), P()),
        check_vma=False,
    )
```

```python
import functools

import jax
import jax.numpy as jnp
from jax import lax
from jax.experimental import pallas as pl
from jax.experimental.pallas import tpu as pltpu
from jax.sharding import PartitionSpec as P


ens_weight = 0.8
static_weight = 0.5
block_lon = 8
block_lat = 16
LIMIT = 44
plan = (2, 4, 4, 4, 2, 2, 2)
f32 = jnp.float32
bf16 = jnp.bfloat16


def my_partner(place):
    return lax.axis_index("lev") ^ place


def shift_by(axis, amount):
    count = lax.axis_size(axis)
    return [(i, (i + amount) % count) for i in range(count)]


def vmem():
    return pl.BlockSpec(memory_space=pltpu.VMEM)


def anywhere():
    return pl.BlockSpec(memory_space=pl.ANY)


def params(count=0):
    return pltpu.CompilerParams(vmem_limit_bytes=(58 if count > 20 else LIMIT) * 2**20)


def smem():
    return pl.BlockSpec(memory_space=pltpu.SMEM)


def cost(flops, nbytes):
    return pl.CostEstimate(flops=int(flops), bytes_accessed=int(nbytes), transcendentals=0)


def lane_groups(shape, width):
    return lax.broadcasted_iota(jnp.int32, shape, len(shape) - 1) // width


def regroup(sources, quarter, parts, width):
    group = lane_groups(sources[0].shape, width)
    out = None
    for p, source in enumerate(sources):
        turn = lax.rem(p - quarter + parts, parts) * width
        moved = pltpu.roll(source, turn, source.ndim - 1)
        out = moved if out is None else jnp.where(group == p, moved, out)
    return out


def pack_kernel(parts, halves, ens_ref, after, *outs):
    levels, columns, lanes = ens_ref.shape[1:]
    width = lanes // parts
    rows = columns // halves
    sources = [ens_ref[p].astype(f32).reshape(levels * columns, lanes) for p in range(parts)]
    for s, out in enumerate(outs):
        packed = regroup(sources, my_partner(s), parts, width)
        packed = packed.reshape(levels, halves, rows, lanes)
        for h in range(halves):
            out[0, h] = packed[:, h].reshape(levels * rows, lanes).astype(bf16)


def pack(ens, start, count, parts, halves, after):
    _, levels, columns, lanes = ens.shape
    rows = levels * columns // halves
    shape = jax.ShapeDtypeStruct((count, halves, rows, lanes), bf16)
    return pl.pallas_call(
        functools.partial(pack_kernel, parts, halves),
        grid=(count,),
        in_specs=[
            pl.BlockSpec((parts, levels, columns, lanes), lambda i: (start + i, 0, 0, 0)),
            anywhere(),
        ],
        out_specs=[pl.BlockSpec((1, halves, rows, lanes), lambda i: (i, 0, 0, 0))] * parts,
        out_shape=[shape] * parts,
        cost_estimate=cost(count * 4e6, count * parts * halves * rows * lanes * 4),
        compiler_params=params(99),
        name="pack",
    )(ens, after)


def ceil_to(x, unit):
    return -(-x // unit) * unit


def message_rows(levels, half_rows, slots, lanes):
    loc = 2 * half_rows
    stat = loc + ceil_to(levels, 16)
    return 0, half_rows, loc, stat, stat + ceil_to(levels, 16), levels * slots // lanes


def pack_small_kernel(
    parts, halves, first, field_ref, sdev_ref, vert_ref, loc_ref, stat_ref, after, *outs
):
    *outs, flat_ref = outs
    levels, columns, lanes = field_ref.shape
    width = lanes // parts
    rows = columns // halves
    slots = vert_ref.shape[0]
    sources = []
    for h in range(halves):
        for ref in (field_ref, sdev_ref):
            sources.append(ref[:, h * rows : (h + 1) * rows, :].reshape(levels * rows, lanes))
    flat = vert_ref[...].T
    flat_ref[...] = jnp.concatenate(
        [flat[:, t : t + lanes] for t in range(0, slots, lanes)], axis=0
    ).astype(bf16)
    for s, out in enumerate(outs):
        high, low = split(regroup(sources, my_partner(s), parts, width))
        out[first[0] : first[1], :] = high
        out[first[1] : first[2], :] = low
        for begin, ref in ((first[2], loc_ref), (first[3], stat_ref)):
            out[begin : begin + ceil_to(levels, 16), :] = jnp.zeros(
                (ceil_to(levels, 16), lanes), bf16
            )
            out[begin : begin + levels, : ref.shape[1]] = ref[...]


def pack_small(field, sdev, vert, loc, stat, parts, halves, after):
    levels, columns, lanes = field.shape
    first = message_rows(levels, levels * columns // halves, vert.shape[0], lanes)
    return pl.pallas_call(
        functools.partial(pack_small_kernel, parts, halves, first),
        in_specs=[vmem()] * 5 + [anywhere()],
        out_specs=[vmem()] * (parts + 1),
        out_shape=[jax.ShapeDtypeStruct((first[-2], lanes), bf16)] * parts
        + [jax.ShapeDtypeStruct((first[-1], lanes), bf16)],
        compiler_params=params(),
        name="pack_small",
    )(field, sdev, vert, loc, stat, after)


def spread_kernel(parts, halves, levels, first, after, *refs):
    messages, (wide_field, wide_sdev, left_end, right_end, loc, stat) = (
        refs[:parts],
        refs[parts:],
    )
    rows = wide_field.shape[1] // parts
    lanes = messages[0].shape[1]
    width = lanes // parts
    group = lane_groups((rows, lanes), width)
    ends = (left_end, right_end)
    for s, message in enumerate(messages):
        x = message[:rows, :].astype(f32) + message[rows : 2 * rows, :].astype(f32)
        for h in range(halves):
            wide = []
            for t in range(2):
                one = jnp.where(group == 2 * h + t, x, 0.0)
                both = one
                for k in range(1, parts):
                    both = both + pltpu.roll(one, k * width, 1)
                wide.append(both)
            wide_field[h, s * rows : (s + 1) * rows, :] = wide[0]
            wide_sdev[h, s * rows : (s + 1) * rows, :] = wide[1]
            ends[h][0, s * rows : (s + 1) * rows, :] = (wide[0] * wide[1]).astype(bf16)
    for begin, out in ((first[2], loc), (first[3], stat)):
        out[...] = jnp.concatenate(
            [m[begin : begin + ceil_to(levels, 16), :].astype(f32)[:levels] for m in messages],
            axis=0,
        ).astype(bf16)


def spread(messages, levels, rows, slots, parts, halves, after):
    lanes = messages[0].shape[1]
    first = message_rows(levels, rows, slots, lanes)
    wide = jax.ShapeDtypeStruct((halves, parts * rows, lanes), f32)
    end = jax.ShapeDtypeStruct((1, parts * rows, lanes), bf16)
    matrix = jax.ShapeDtypeStruct((parts * levels, lanes), bf16)
    return pl.pallas_call(
        functools.partial(spread_kernel, parts, halves, levels, first),
        in_specs=[anywhere()] + [vmem()] * parts,
        out_specs=[vmem()] * 6,
        out_shape=[wide, wide, end, end, matrix, matrix],
        compiler_params=params(),
        name="spread",
    )(after, *messages)


def product_kernel(parts, field_ref, *refs):
    xs, ends = refs[:parts], refs[-2:]
    count, _, rows, _ = xs[0].shape
    for s, x in enumerate(xs):
        here = slice(s * rows, (s + 1) * rows)
        for h, end in enumerate(ends):
            scale = field_ref[h, here, :]
            for k in range(count):
                end[k, here, :] = (x[k, h].astype(f32) * scale).astype(bf16)


def product(wide_field, xs, after):
    parts = len(xs)
    count, halves, rows, lanes = xs[0].shape
    step = 2 if count % 2 == 0 else 1
    end = jax.ShapeDtypeStruct((count, parts * rows, lanes), bf16)
    return pl.pallas_call(
        functools.partial(product_kernel, parts),
        grid=(count // step,),
        in_specs=[pl.BlockSpec(wide_field.shape, lambda i: (0, 0, 0))]
        + [pl.BlockSpec((step, halves, rows, lanes), lambda i: (i, 0, 0, 0))] * parts
        + [anywhere()] * len(after),
        out_specs=[pl.BlockSpec((step, parts * rows, lanes), lambda i: (i, 0, 0))] * halves,
        out_shape=[end] * halves,
        cost_estimate=cost(count * 1e6, count * halves * parts * rows * lanes * 4),
        compiler_params=params(count),
        name="product",
    )(wide_field, *xs, *after)


def filter_kernel(pair, has_total, matrix_ref, left, first, last, right, *refs):
    refs = list(refs)
    stack = refs.pop()
    total_out = refs.pop()
    total_in = refs.pop() if has_total else None
    xs = refs
    rows, lanes = first.shape[1:]

    @pl.when(pl.program_id(0) == 0)
    def _():
        if has_total:
            total_out[...] = total_in[...]
        else:
            total_out[...] = jnp.zeros_like(total_out)

    for n, ref in enumerate((left, first, last, right)):
        for k in range(pair):
            stack[n * rows : (n + 1) * rows, k * lanes : (k + 1) * lanes] = ref[k]
    for h in range(total_out.shape[0]):
        y = jnp.dot(
            matrix_ref[...], stack[h * rows : (h + 3) * rows, :], preferred_element_type=f32
        )
        piece = rows // len(xs)
        for s, x in enumerate(xs):
            here = slice(s * piece, (s + 1) * piece)
            add = total_out[h, here, :]
            for k in range(pair):
                add = add + x[k, h].astype(f32) * y[here, k * lanes : (k + 1) * lanes]
            total_out[h, here, :] = add


def filtered(matrix, left, first, last, right, xs, total):
    count, rows, lanes = first.shape
    pair = 2 if count % 2 == 0 else 1
    halves = 2
    piece = rows // len(xs)
    edge = pl.BlockSpec((pair, rows, lanes), lambda i: (i, 0, 0))
    whole = pl.BlockSpec((halves, rows, lanes), lambda i: (0, 0, 0))
    return pl.pallas_call(
        functools.partial(filter_kernel, pair, total is not None),
        grid=(count // pair,),
        in_specs=[pl.BlockSpec(matrix.shape, lambda i: (0, 0))]
        + [edge] * 4
        + [pl.BlockSpec((pair, halves, piece, lanes), lambda i: (i, 0, 0, 0))] * len(xs)
        + ([whole] if total is not None else []),
        out_specs=whole,
        out_shape=jax.ShapeDtypeStruct((halves, rows, lanes), f32),
        scratch_shapes=[pltpu.VMEM((4 * rows, pair * lanes), bf16)],
        cost_estimate=cost(
            2 * halves * matrix.shape[0] * matrix.shape[1] * lanes * count,
            count * rows * lanes * 12,
        ),
        compiler_params=params(count),
        name="filtered",
    )(matrix, left, first, last, right, *xs, *([total] if total is not None else []))


def fold_kernel(parts, block_rows, total_ref, static_ref, blocks_ref, mixed):
    halves, rows, lanes = total_ref.shape
    width = lanes // parts
    levels = rows // block_lon
    for h in range(halves):
        x = ens_weight * total_ref[h] + (static_weight / parts) * static_ref[h]
        folded = x
        for k in range(1, parts):
            folded = folded + pltpu.roll(x, k * width, 1)
        mixed[h * rows : (h + 1) * rows, :] = folded
    group = lane_groups((levels, lanes), block_lat)
    for h in range(halves):
        strips = [mixed[pl.ds(h * rows + i, levels, stride=block_lon), :] for i in range(block_lon)]
        for b in range(block_rows):
            out = None
            for i, strip in enumerate(strips):
                moved = pltpu.roll(strip, ((i - b) * block_lat) % lanes, 1)
                out = moved if out is None else jnp.where(group == i, moved, out)
            blocks_ref[b, h * levels : (h + 1) * levels, :] = out


def fold(total, static, parts):
    halves, rows, lanes = total.shape
    levels = rows // block_lon
    block_rows = lanes // parts // block_lat
    return pl.pallas_call(
        functools.partial(fold_kernel, parts, block_rows),
        in_specs=[vmem()] * 2,
        out_specs=vmem(),
        out_shape=jax.ShapeDtypeStruct((block_rows, halves * levels, lanes), f32),
        scratch_shapes=[pltpu.VMEM((halves * rows, lanes), f32)],
        cost_estimate=cost(2e6, 2e6),
        compiler_params=params(),
        name="fold",
    )(total, static)


def split(x):
    high = x.astype(bf16)
    return high, (x - high.astype(f32)).astype(bf16)


def horiz_kernel(horiz_ref, high, low, high_t, low_t):
    hi, lo = split(horiz_ref[...])
    high[...] = hi
    low[...] = lo
    flipped_hi, flipped_lo = split(horiz_ref[...].T)
    high_t[...] = flipped_hi
    low_t[...] = flipped_lo


def horiz_parts(horiz):
    slots, cells = horiz.shape
    return pl.pallas_call(
        horiz_kernel,
        in_specs=[vmem()],
        out_specs=[vmem()] * 4,
        out_shape=[jax.ShapeDtypeStruct((slots, cells), bf16)] * 2
        + [jax.ShapeDtypeStruct((cells, slots), bf16)] * 2,
        cost_estimate=cost(1e6, 2e6),
        compiler_params=params(),
        name="horiz_parts",
    )(horiz)


def product3(a, high, low):
    a_high, a_low = split(a)
    dot = functools.partial(jnp.dot, preferred_element_type=f32)
    return dot(a_high, high) + (dot(a_low, high) + dot(a_high, low))


def vert_kernel(*refs):
    *verts, out = refs
    lanes = verts[0].shape[1]
    piece = out.shape[0] // len(verts)
    for s, ref in enumerate(verts):
        rows = ref[...].astype(f32)
        for t in range(out.shape[1] // lanes):
            here = slice(t * piece, (t + 1) * piece)
            out[s * piece : (s + 1) * piece, t * lanes : (t + 1) * lanes] = rows[here]


def join_vert(verts, levels, slots):
    return pl.pallas_call(
        vert_kernel,
        in_specs=[vmem()] * len(verts),
        out_specs=vmem(),
        out_shape=jax.ShapeDtypeStruct((len(verts) * levels, slots), f32),
        cost_estimate=cost(1e6, 1e6),
        compiler_params=params(),
        name="join_vert",
    )(*verts)


def block_picks(ids, halves, block_rows, lat_blocks):
    base = lax.axis_index("lev") * block_rows
    return [[ids == h * lat_blocks + base + b for b in range(block_rows)] for h in range(halves)]


def depart_kernel(
    halves, lat_blocks, blocks_ref, vert_ref, high_t, low_t, ids_ref, value_ref, rinv_ref,
    dep_ref, share_ref
):
    block_rows, stacked, cells = blocks_ref.shape
    levels = stacked // halves
    vert = vert_ref[...]
    picks = block_picks(ids_ref[...], halves, block_rows, lat_blocks)
    mine = None
    hx = jnp.zeros(ids_ref.shape, f32)
    for b in range(block_rows):
        projected = product3(blocks_ref[b], high_t[...], low_t[...])
        for h in range(halves):
            one = jnp.sum(projected[h * levels : (h + 1) * levels] * vert, axis=0, keepdims=True)
            hx = jnp.where(picks[h][b], one, hx)
            mine = picks[h][b] if mine is None else mine | picks[h][b]
    miss = hx - value_ref[...]
    dep = jnp.where(mine, rinv_ref[...] * miss, 0.0)
    dep_ref[...] = dep
    total = 0.5 * jnp.sum(dep * miss, axis=1, keepdims=True)
    slot = lax.axis_index("lon") * lax.axis_size("lev") + lax.axis_index("lev")
    spot = lax.broadcasted_iota(jnp.int32, share_ref.shape, 0) * cells
    spot = spot + lax.broadcasted_iota(jnp.int32, share_ref.shape, 1)
    share_ref[...] = jnp.where(spot == slot, jnp.broadcast_to(total, share_ref.shape), 0.0)


def adjoint_kernel(
    parts, halves, lat_blocks, blocks_ref, vert_ref, high, low, ids_ref, dep_ref, *outs
):
    block_rows, stacked, _ = blocks_ref.shape
    levels = stacked // halves
    piece = levels // parts
    vert = vert_ref[...]
    dep = dep_ref[...]
    picks = block_picks(ids_ref[...], halves, block_rows, lat_blocks)
    both = [[], []]
    for b in range(block_rows):
        weights = jnp.concatenate(
            [vert * jnp.where(picks[h][b], dep, 0.0) for h in range(halves)], axis=0
        )
        both[0].append(blocks_ref[b])
        both[1].append(product3(weights, high[...], low[...]))
    for s, ref in enumerate(outs):
        pieces = [
            x[h * levels + s * piece : h * levels + (s + 1) * piece]
            for b in range(block_rows)
            for x in (both[0][b], both[1][b])
            for h in range(halves)
        ]
        ref[...] = jnp.concatenate(pieces, axis=0).astype(bf16)


def observe(blocks, vert, horiz, ids, value, rinv, parts, halves, lat_blocks):
    high, low, high_t, low_t = horiz
    block_rows, stacked, cells = blocks.shape
    dep, share = pl.pallas_call(
        functools.partial(depart_kernel, halves, lat_blocks),
        in_specs=[vmem()] * 7,
        out_specs=[vmem()] * 2,
        out_shape=[
            jax.ShapeDtypeStruct(ids.shape, f32),
            jax.ShapeDtypeStruct((8, cells), f32),
        ],
        cost_estimate=cost(1e9, 4e6),
        compiler_params=params(),
        name="depart",
    )(blocks, vert, high_t, low_t, ids, value, rinv)
    back = jax.ShapeDtypeStruct((2 * block_rows * stacked // parts, cells), bf16)
    backs = pl.pallas_call(
        functools.partial(adjoint_kernel, parts, halves, lat_blocks),
        in_specs=[vmem()] * 6,
        out_specs=[vmem()] * parts,
        out_shape=[back] * parts,
        cost_estimate=cost(1e9, 4e6),
        compiler_params=params(),
        name="adjoint",
    )(blocks, vert, high, low, ids, dep)
    return share, backs


def unpack_kernel(halves, levels, *refs):
    *backs, increment_ref, adjoint_ref, strips = refs
    rows, lanes = backs[0].shape
    width = lanes // len(backs)
    block_rows = width // block_lat
    count = rows // block_rows
    group = lane_groups((count, lanes), block_lat)
    pieces = []
    for s, ref in enumerate(backs):
        x = ref[...].astype(f32)
        for b in range(block_rows):
            place = my_partner(s) * width + b * block_lat
            pieces.append((place, x[b * count : (b + 1) * count]))
    for i in range(block_lon):
        strip = None
        for place, x in pieces:
            x = jnp.where(group == i, x, 0.0)
            x = pltpu.roll(x, lax.rem(place + lanes - i * block_lat, lanes), 1)
            strip = x if strip is None else strip + x
        strips[i * count : (i + 1) * count, :] = strip
    for n, out_ref in enumerate((increment_ref, adjoint_ref)):
        for h in range(halves):
            for l in range(levels):
                row = (n * halves + h) * levels + l
                first = (l * halves + h) * block_lon
                out_ref[first : first + block_lon, :] = strips[
                    pl.ds(row, block_lon, stride=count), :
                ]


def unpack(backs, levels, columns, lanes):
    halves = columns // block_lon
    outs = pl.pallas_call(
        functools.partial(unpack_kernel, halves, levels),
        in_specs=[vmem()] * len(backs),
        out_specs=[vmem()] * 2,
        out_shape=[jax.ShapeDtypeStruct((levels * columns, lanes), f32)] * 2,
        scratch_shapes=[pltpu.VMEM((2 * levels * columns, lanes), f32)],
        cost_estimate=cost(1e7, 1e6),
        compiler_params=params(),
        name="unpack",
    )(*backs)
    return [x.reshape(levels, columns, lanes) for x in outs]


def exchange(blocks):
    count = lax.axis_size("lev")
    return [blocks[0]] + [
        lax.ppermute(blocks[place], "lev", [(i, i ^ place) for i in range(count)])
        for place in range(1, count)
    ]


def bands_kernel(rows, span, lon_ref, static_ref, *outs):
    for taper_ref, out in zip((lon_ref, static_ref), outs):
        column = lax.broadcasted_iota(jnp.int32, out.shape, 1)
        offset = column // span * rows + column % rows
        offset = offset - lax.broadcasted_iota(jnp.int32, out.shape, 0)
        band = jnp.zeros(out.shape, f32)
        for d in range(2 * rows + 1):
            band = jnp.where(offset == d, taper_ref[d], band)
        out[...] = band


def bands(lon_taper, static_taper, rows, span):
    shape = jax.ShapeDtypeStruct((rows, 3 * span), f32)
    return pl.pallas_call(
        functools.partial(bands_kernel, rows, span),
        in_specs=[smem()] * 2,
        out_specs=[vmem()] * 2,
        out_shape=[shape] * 2,
        compiler_params=params(),
        name="bands",
    )(lon_taper.astype(f32), static_taper.astype(f32))


def total_of(x, axis):
    reach = 1
    while reach < lax.axis_size(axis):
        pairs = [(i, i ^ reach) for i in range(lax.axis_size(axis))]
        x = x + lax.ppermute(x, axis, pairs)
        reach *= 2
    return x


def operator(vert_rows, band, parts, levels, rows):
    total = parts * levels
    span = total * rows
    column = jnp.arange(3 * span)
    source = column % span // rows
    owner = my_partner(source // levels)
    pick = (jnp.arange(vert_rows.shape[1])[:, None] == (owner * levels + source % levels)[None, :])
    wide = jnp.dot(vert_rows, pick.astype(bf16), preferred_element_type=f32).astype(bf16)
    grow = (jnp.arange(span)[:, None] // rows == jnp.arange(total)[None, :]).astype(bf16)
    tall = jnp.dot(grow, wide, preferred_element_type=f32)
    return (tall.reshape(total, rows, 3 * span) * band[None]).astype(bf16).reshape(span, 3 * span)


def filters_after(chunk, chunks):
    ahead = chunks - 4
    if chunk == chunks - 1:
        return range(ahead, chunks)
    return range(chunk - 1, chunk) if 1 <= chunk <= ahead else range(0)


def chunk_sizes(groups):
    ends = [groups * sum(plan[: n + 1]) // sum(plan) for n in range(len(plan))]
    return [end - begin for begin, end in zip([0] + ends, ends)]


def body(
    field,
    ens,
    sdev,
    lon_taper,
    static_taper,
    loc_vert,
    static_vert,
    obs_block,
    obs_value,
    obs_rinv,
    obs_horiz,
    obs_vert,
):
    members, levels, columns, lanes = ens.shape
    parts = lax.axis_size("lev")
    rows = lon_taper.shape[0] // 2
    halves = columns // rows
    lat_blocks = lanes // block_lat
    slots = obs_block.shape[0]

    sizes = chunk_sizes(members // parts)
    starts = [sum(sizes[:n]) for n in range(len(sizes))]
    first_pack = pack(ens, starts[0], sizes[0], parts, halves, lon_taper)
    *messages, vert_rows = pack_small(
        field, sdev, obs_vert, loc_vert, static_vert, parts, halves, first_pack[0]
    )
    half_rows = levels * rows
    received = [exchange(first_pack)]
    after = messages[0]
    messages = exchange(messages)
    for n in range(1, len(sizes)):
        packed = pack(ens, starts[n], sizes[n], parts, halves, after)
        after = packed[0]
        received.append(exchange(packed))

    verts = exchange([vert_rows] * parts)
    wide_field, wide_sdev, static_first, static_last, loc_all, stat_all = spread(
        messages, levels, half_rows, slots, parts, halves, after
    )
    lon_band, static_band = bands(lon_taper, static_taper, rows, parts * half_rows)
    loc_matrix = operator(loc_all, lon_band, parts, levels, rows)
    stat_matrix = operator(stat_all, static_band, parts, levels, rows)
    horiz = horiz_parts(obs_horiz)

    def halo(first, last):
        left = lax.ppermute(last, "lon", shift_by("lon", 1))
        right = lax.ppermute(first, "lon", shift_by("lon", -1))
        return left, right

    left, right = halo(static_first, static_last)
    static = filtered(stat_matrix, left, static_first, static_last, right, [wide_sdev[None]], None)
    total = None
    ready = []
    after = [static_first]
    for n, xs in enumerate(received):
        first, last = product(wide_field, xs, after)
        left, right = halo(first, last)
        ready.append((left, first, last, right, xs))
        after = [first] if n else [first, static]
        for m in filters_after(n, len(received)):
            total = filtered(loc_matrix, *ready[m], total)
            after = [total]

    blocks = fold(total, static, parts)

    nblk = columns // block_lon * lat_blocks
    ids = jnp.where(obs_block >= 0, obs_block - lax.axis_index("lon") * nblk, -1)
    share, backs = observe(
        blocks, join_vert(verts, levels, slots), horiz, ids[None], obs_value[None], obs_rinv[None],
        parts, halves, lat_blocks,
    )
    backs = exchange(backs)
    shares = total_of(total_of(share, "lon"), "lev")
    obs_cost = jnp.sum(shares)

    increment, adjoint_field = unpack(backs, levels, columns, lanes)
    return (increment, adjoint_field, obs_cost)


def solution(mesh):
    return jax.shard_map(
        body,
        mesh=mesh,
        in_specs=(
            P("lev", "lon", None),
            P(None, "lev", "lon", None),
            P("lev", "lon", None),
            P(),
            P(),
            P("lev", None),
            P("lev", None),
            P("lon"),
            P("lon"),
            P("lon"),
            P("lon", None),
            P("lon", "lev"),
        ),
        out_specs=(P("lev", "lon", None), P("lev", "lon", None), P()),
        check_vma=False,
    )
```
